32 devices in a mesh: gx: 8 (over z, y), gy: 4 (over x, core).
Axes of the slice: x: 2, y: 2, z: 4, core: 2. Of those that a mesh axis runs over, the one named last changes fastest.
Arguments:
- forces: float32 [3, 128, 128, 256], P(None, 'gx', 'gy'), may hold values from -8 to 8
- pressure_prev: float32 [128, 128, 256], P('gx', 'gy'), may hold values from -8 to 8
Outputs:
- pressure: float32 [128, 128, 256], P('gx', 'gy')
- residual: float32 [128, 128, 256], P('gx', 'gy')
The draws below stay inside these ranges and needn't reach their ends.
All inputs are finite; a program needn't handle non-finite values.
Results may differ from the reference program's by a relative error of at most 0.0003.
Values sent between devices are 32-bit elements; how exact they have to be, the bound alone decides.
A program may use at most 64 MiB of HBM per device.

```python
import jax
import jax.numpy as jnp
from jax import lax

NZ = 256
LEVELS = 5
SWEEPS = 2
COARSE_SWEEPS = 4
CYCLES = 2
NX = 128
NY = 128


def draw_pressure_prev(key, part):
    noise_key = jax.random.fold_in(key, 11)
    profile_key = jax.random.fold_in(key, 23)
    profile = 2.5 * jax.random.normal(profile_key, (NZ,), jnp.float32)
    noise = jax.random.normal(noise_key, (NX, NY, NZ), jnp.float32)
    return jnp.clip(noise + profile[None, None, :], -8.0, 8.0).astype(jnp.float32)


def block_scale(key, dims, shards, low, top_value):
    loudness, own = 1.0, jax.random.fold_in(key, 6)
    for dim, parts in shards:
        heights = jnp.exp(jax.random.uniform(jax.random.fold_in(own, dim), (parts,), jnp.float32, low / len(shards), top_value / len(shards)))
        loudness = loudness * jnp.repeat(heights, dims[dim] // parts).reshape([-1 if axis == dim else 1 for axis in range(len(dims))])
    return loudness


def normal_values(own_key, shape, spread, most, pieces=(), kind=jnp.bfloat16):
    gain = block_scale(own_key, shape, pieces, -0.22, 0.18) if pieces else 1.0
    drawn = jax.random.normal(own_key, shape, jnp.float32) * spread * gain
    return jnp.minimum(jnp.maximum(drawn, -most), most).astype(kind)


def setup_inputs(seed: int = 0) -> dict:
    splits = jax.random.split(jax.random.key(seed), 3)
    return {
        "forces": normal_values(splits[0], (3, NX, NY, NZ), 1.0, 8.0, ((1, 8), (2, 4)), jnp.float32),
        "pressure_prev": draw_pressure_prev(jax.random.fold_in(splits[2], 71), 0),
    }


OMEGA = 0.8

def vertical(values):
    padded = jnp.pad(values, ((0, 0), (0, 0), (1, 1)))
    return padded[:, :, 2:] + padded[:, :, :-2]

def operate_padded(padded, weight):
    center = padded[1:-1, 1:-1]
    beside = padded[2:, 1:-1] + padded[:-2, 1:-1] + padded[1:-1, 2:] + padded[1:-1, :-2]
    return weight * (4.0 * center - beside) + (2.0 * center - vertical(center))

def relax(padded, source, weight):
    center = padded[1:-1, 1:-1]
    return center + OMEGA * (source - operate_padded(padded, weight)) / (4.0 * weight + 2.0)

def wrapped(values):
    return jnp.pad(values, ((1, 1), (1, 1), (0, 0)), mode='wrap')

def restrict(residual_now):
    rows_x, rows_y, depth = residual_now.shape
    return 0.25 * residual_now.reshape(rows_x // 2, 2, rows_y // 2, 2, depth).sum(axis=(1, 3))

def prolong(correction):
    return jnp.repeat(jnp.repeat(correction, 2, axis=0), 2, axis=1)

def mean_mode(values, source):
    depth = source.shape[2]
    column = jnp.mean(source, axis=(0, 1))
    lower = jnp.concatenate([jnp.zeros((1,), source.dtype), -jnp.ones((depth - 1,), source.dtype)])
    upper = jnp.concatenate([-jnp.ones((depth - 1,), source.dtype), jnp.zeros((1,), source.dtype)])
    middle = 2.0 * jnp.ones((depth,), source.dtype)
    profile = lax.linalg.tridiagonal_solve(lower, middle, upper, column[:, None])[:, 0]
    return values + profile[None, None, :]

def whole_cycle(values, source, level_index):
    weight = 0.25 ** level_index
    if level_index == LEVELS - 1:
        values = mean_mode(values, source)
        for sweep_index in range(COARSE_SWEEPS):
            values = relax(wrapped(values), source, weight)
        return values
    for sweep_index in range(SWEEPS):
        values = relax(wrapped(values), source, weight)
    residual_now = source - operate_padded(wrapped(values), weight)
    coarse_source = restrict(residual_now)
    correction = whole_cycle(jnp.zeros_like(coarse_source), coarse_source, level_index + 1)
    values = values + prolong(correction)
    for sweep_index in range(SWEEPS):
        values = relax(wrapped(values), source, weight)
    return values

def reference(forces, pressure_prev):
    force_x, force_y, force_z = (forces[0], forces[1], forces[2])
    behind_x = jnp.roll(force_x, 1, axis=0)
    behind_y = jnp.roll(force_y, 1, axis=1)
    behind_z = jnp.pad(force_z[:, :, :-1], ((0, 0), (0, 0), (1, 0)))
    source = behind_x - force_x + (behind_y - force_y) + (behind_z - force_z)
    pressure = pressure_prev
    for cycle_index in range(CYCLES):
        pressure = whole_cycle(pressure, source, 0)
    residual = source - operate_padded(wrapped(pressure), 1.0)
    return (pressure, residual)
```

```python
import functools

import numpy as np

import jax
import jax.numpy as jnp
from jax import lax
from jax.experimental import pallas as pl
from jax.experimental.pallas import tpu as pltpu
from jax.sharding import PartitionSpec as P

OMEGA = 0.8
LEVELS = 5
CYCLES = 2
COARSE_SWEEPS = 4
PAD = 8
SUB = 8
LANES = 128
MESH = pl.DeviceIdType.MESH
EXACT = lax.Precision.HIGHEST


def loop(count, body):
    def step(i, carry):
        body(i)
        return carry

    lax.fori_loop(0, count, step, 0)


def lateral_rows(v, r, count, by):
    block = v[pl.ds(r, count + 2)]
    c = block[1:-1]
    width = c.shape[1]
    sides = pltpu.roll(c, 1, 1) + pltpu.roll(c, width - 1, 1)
    around = (block[:-2] + block[2:] + sides)[:, PAD : PAD + by]
    return 4.0 * c[:, PAD : PAD + by] - around


class Level:
    def __init__(self, index, rows, rate):
        self.rows, self.rate, self.shift = rows, rate, 2**index
        self.weight = 0.25**index
        self.k = OMEGA / (4.0 * self.weight + 2.0)
        self.unit = min(rows, 8)

    def sides(self, c):
        axis = c.ndim - 1
        return pltpu.roll(c, self.shift, axis) + pltpu.roll(c, c.shape[axis] - self.shift, axis)

    def relax(self, c, lateral, f):
        keep = 1.0 - self.k * (4.0 * self.weight + self.rate)
        return keep * c + (self.k * self.weight) * lateral + self.k * f

    def begin(self, f, lateral):
        keep = self.k * (2.0 - self.k * (4.0 * self.weight + self.rate))
        return keep * f + (self.k * self.k * self.weight) * lateral

    def remainder(self, c, lateral, f):
        return (f - self.rate * c) - self.weight * (4.0 * c - lateral)

    def restrict(self, r):
        pairs = r.reshape((r.shape[0] // 2, 2) + r.shape[1:])
        s = pairs[:, 0] + pairs[:, 1]
        width = s.shape[2]
        lane = lax.broadcasted_iota(jnp.int32, s.shape, 2)
        odd = (lane & self.shift) != 0
        other = jnp.where(odd, pltpu.roll(s, self.shift, 2), pltpu.roll(s, width - self.shift, 2))
        return 0.25 * (s + other)

    def each(self, body):
        loop(self.rows // self.unit, lambda i: body(pl.multiple_of(i * self.unit, self.unit)))

    def around(self, ref, x):
        block = ref[pl.ds(x, self.unit + 2)]
        c = block[1:-1]
        return c, (block[:-2] + block[2:]) + self.sides(c)

    def ghosts(self, ref):
        ref[0] = ref[self.rows]
        ref[self.rows + 1] = ref[1]

    def sweep(self, v, f, dst):
        def body(x):
            c, lateral = self.around(v, x)
            dst[pl.ds(1 + x, self.unit)] = self.relax(c, lateral, f[pl.ds(1 + x, self.unit)])

        self.each(body)
        self.ghosts(dst)

    def sweep_twice_from_zero(self, f, dst):
        def body(x):
            c, lateral = self.around(f, x)
            dst[pl.ds(1 + x, self.unit)] = self.begin(c, lateral)

        self.each(body)
        self.ghosts(dst)

    def restricted(self, v, f, dst):
        def body(x):
            c, lateral = self.around(v, x)
            r = self.remainder(c, lateral, f[pl.ds(1 + x, self.unit)])
            dst[pl.ds(1 + x // 2, self.unit // 2)] = self.restrict(r)

        self.each(body)
        dst[0] = dst[self.rows // 2]
        dst[self.rows // 2 + 1] = dst[1]

    def corrected_sweep(self, v, e, f, dst):
        def body(x):
            block = v[pl.ds(x, self.unit + 2)]
            half = e[pl.ds(x // 2, self.unit // 2 + 2)]
            pieces = [half[i] for i in range(self.unit // 2 + 2)]
            twice = [pieces[0]] + [p for p in pieces[1:-1] for _ in range(2)] + [pieces[-1]]
            block = block + jnp.stack(twice)
            c = block[1:-1]
            lateral = (block[:-2] + block[2:]) + self.sides(c)
            dst[pl.ds(1 + x, self.unit)] = self.relax(c, lateral, f[pl.ds(1 + x, self.unit)])

        self.each(body)
        self.ghosts(dst)

    def whole(self, c):
        up = jnp.concatenate([c[-1:], c[:-1]], axis=0)
        down = jnp.concatenate([c[1:], c[:1]], axis=0)
        return (up + down) + self.sides(c)


def kernel(
    nx, ny,
    forces, pressure, sine_in, rates_in, out_p, out_r,
    fx, fy, fz, pa, da, r0, sine, rates, sb, rb, sb2, rb2,
    f0, a0, b0, f1, a1, b1, f2, a2, b2, f3, a3, b3, f4, a4,
    local_sem, plane_send, plane_recv, halo_send, halo_recv,
    go_send, go_recv, back_send, back_recv,
):
    mx, my = lax.axis_index("gx"), lax.axis_index("gy")
    n = nx * ny
    me = mx * ny + my
    bx, by, depth = pressure.shape
    tx = LANES // by
    tiles = bx // tx

    loads = [
        pltpu.make_async_copy(forces.at[0], fx.at[pl.ds(1, bx)], local_sem.at[0]),
        pltpu.make_async_copy(forces.at[1], fy.at[:, pl.ds(PAD, by)], local_sem.at[1]),
        pltpu.make_async_copy(pressure, pa.at[pl.ds(1, bx), pl.ds(PAD, by)], local_sem.at[2]),
        pltpu.make_async_copy(forces.at[2], fz, local_sem.at[3]),
        pltpu.make_async_copy(sine_in, sine, local_sem.at[4]),
        pltpu.make_async_copy(rates_in, rates, local_sem.at[5]),
    ]
    for load in loads:
        load.start()

    def device(d):
        return d // ny, lax.rem(d, ny)

    barrier = pltpu.get_barrier_semaphore()

    def greet(j):
        pl.semaphore_signal(
            barrier, inc=1, device_id=device(lax.rem(me + 1 + j, n)), device_id_type=MESH
        )

    loop(n - 1, greet)
    pl.semaphore_wait(barrier, n - 1)

    right, left = lax.rem(mx + 1, nx), lax.rem(mx + nx - 1, nx)
    above, below = lax.rem(my + 1, ny), lax.rem(my + ny - 1, ny)

    def remote(src, dst, send, recv, to):
        copy = pltpu.make_async_remote_copy(
            src_ref=src, dst_ref=dst, send_sem=send, recv_sem=recv,
            device_id=to, device_id_type=MESH,
        )
        copy.start()
        return copy

    def halo(ref, turn):
        inner = pl.ds(PAD, by)
        rows = pl.ds(1, bx)

        def strip(d, src, dst, to):
            return remote(src, dst, halo_send.at[turn, d], halo_recv.at[turn, d], to)

        return [
            strip(0, ref.at[pl.ds(bx, 1), inner], ref.at[pl.ds(0, 1), inner], (right, my)),
            strip(1, ref.at[pl.ds(1, 1), inner], ref.at[pl.ds(bx + 1, 1), inner], (left, my)),
            strip(2, ref.at[rows, pl.ds(PAD + by - 1, 1)], ref.at[rows, pl.ds(PAD - 1, 1)], (mx, above)),
            strip(3, ref.at[rows, pl.ds(PAD, 1)], ref.at[rows, pl.ds(PAD + by, 1)], (mx, below)),
        ]

    for load in loads[:3]:
        load.wait()
    early = halo(pa, 0)
    early.append(
        remote(fx.at[pl.ds(bx, 1)], fx.at[pl.ds(0, 1)], plane_send.at[0], plane_recv.at[0], (right, my))
    )
    early.append(
        remote(
            fy.at[:, pl.ds(PAD + by - 1, 1)], fy.at[:, pl.ds(PAD - 1, 1)],
            plane_send.at[1], plane_recv.at[1], (mx, above),
        )
    )
    for load in loads[3:]:
        load.wait()
    for copy in early:
        copy.wait_recv()

    def make_remainder(i):
        r = 2 * i
        x = fx[pl.ds(r, 3)]
        y = fy[pl.ds(r, 2)]
        z = fz[pl.ds(r, 2)]
        lane = lax.broadcasted_iota(jnp.int32, z.shape, 2)
        behind_z = jnp.where(lane == 0, 0.0, pltpu.roll(z, 1, 2))
        behind_y = pltpu.roll(y, 1, 1)[:, PAD:]
        source = (x[:-1] - x[1:]) + (behind_y - y[:, PAD:]) + (behind_z - z)
        r0[pl.ds(r, 2)] = source - lateral_rows(pa, r, 2, by)

    loop(bx // 2, make_remainder)

    every = rates[...]

    def to_modes(cells):
        return lax.dot_general(
            sine[...], cells.reshape(2 * LANES, depth), (((1,), (1,)), ((), ())),
            preferred_element_type=jnp.float32, precision=EXACT,
        )

    def forward(i):
        r = 2 * tx * i
        modes = to_modes(r0[pl.ds(r, 2 * tx)])
        start = to_modes(pa[pl.ds(1 + r, 2 * tx), PAD : PAD + by])
        for h in range(2):
            half = slice(h * LANES, (h + 1) * LANES)
            sb[:, 2 * i + h] = (modes[:, half] - every * start[:, half]).reshape(n, SUB, LANES)

    loop(tiles // 2, forward)

    def exchange(src, dst, send, recv):
        def message(d, slot):
            return pltpu.make_async_remote_copy(
                src_ref=src.at[d], dst_ref=dst.at[slot], send_sem=send.at[d], recv_sem=recv.at[slot],
                device_id=device(d), device_id_type=MESH,
            )

        def start(j):
            d = lax.rem(me + 1 + j, n)
            message(d, me).start()

        loop(n - 1, start)
        dst[me] = src[me]

        def arrive(j):
            d = lax.rem(me + 1 + j, n)
            message(d, d).wait_recv()

        loop(n - 1, arrive)

        def finish():
            def done(j):
                d = lax.rem(me + 1 + j, n)
                message(d, d).wait_send()

            loop(n - 1, done)

        return finish

    ends = [exchange(sb, rb, go_send, go_recv)]

    def assemble(q):
        gx, t = q // tiles, lax.rem(q, tiles)
        parts = [rb[gx * ny + g, t] for g in range(ny)]
        for i in range(tx):
            row = [part[:, i * by : (i + 1) * by] for part in parts]
            f0[1 + q * tx + i] = jnp.concatenate(row, axis=1)

    loop(nx * tiles, assemble)

    mine = rates[pl.ds(pl.multiple_of(me * SUB, SUB), SUB)]
    lam = jnp.concatenate([mine] * (ny * by // LANES), axis=1)
    rows = nx * bx
    l0, l1, l2, l3, l4 = (Level(i, rows // 2**i, lam) for i in range(LEVELS))
    l0.ghosts(f0)

    for cycle in range(CYCLES):
        if cycle == 0:
            l0.sweep_twice_from_zero(f0, a0)
        else:
            l0.sweep(a0, f0, b0)
            l0.sweep(b0, f0, a0)
        l0.restricted(a0, f0, f1)
        l1.sweep_twice_from_zero(f1, a1)
        l1.restricted(a1, f1, f2)
        l2.sweep_twice_from_zero(f2, a2)
        l2.restricted(a2, f2, f3)
        l3.sweep_twice_from_zero(f3, a3)
        l3.restricted(a3, f3, f4)
        f = f4[pl.ds(1, l4.rows)]
        mean = jnp.sum(jnp.sum(f, axis=0), axis=1, keepdims=True) / (l4.rows * f.shape[2])
        v = jnp.broadcast_to((mean / lam)[None], f.shape)
        for _ in range(COARSE_SWEEPS):
            v = l4.relax(v, l4.whole(v), f)
        a4[pl.ds(1, l4.rows)] = v
        l4.ghosts(a4)
        l3.corrected_sweep(a3, a4, f3, b3)
        l3.sweep(b3, f3, a3)
        l2.corrected_sweep(a2, a3, f2, b2)
        l2.sweep(b2, f2, a2)
        l1.corrected_sweep(a1, a2, f1, b1)
        l1.sweep(b1, f1, a1)
        l0.corrected_sweep(a0, a1, f0, b0)
        l0.sweep(b0, f0, a0)

    def disassemble(q):
        gx, t = q // tiles, lax.rem(q, tiles)
        block = a0[pl.ds(1 + q * tx, tx)]
        for g in range(ny):
            pieces = [block[i][:, g * by : (g + 1) * by] for i in range(tx)]
            sb2[gx * ny + g, t] = jnp.concatenate(pieces, axis=1)

    loop(nx * tiles, disassemble)
    ends.append(exchange(sb2, rb2, back_send, back_recv))

    def backward(mail, i):
        halves = [mail[:, 2 * i + h].reshape(n * SUB, LANES) for h in range(2)]
        cells = lax.dot_general(
            jnp.concatenate(halves, axis=1), sine[...], (((0,), (0,)), ((), ())),
            preferred_element_type=jnp.float32, precision=EXACT,
        )
        return cells.reshape(2 * tx, by, depth)

    def correction(i):
        d = backward(rb2, i)
        da[pl.ds(1 + 2 * tx * i, 2 * tx), PAD : PAD + by] = d
        r = 2 * tx * i
        out_p[pl.ds(r, 2 * tx)] = pa[pl.ds(1 + r, 2 * tx), PAD : PAD + by] + d

    loop(tiles // 2, correction)
    late = halo(da, 1)

    def inner_remainder(d):
        c = rb2[d]
        lane = lax.broadcasted_iota(jnp.int32, c.shape, 2)
        column = lax.rem(lane, by)
        zero = jnp.zeros_like(c[:1])
        after = pltpu.roll(c, LANES - by, 2)
        after = jnp.where(lane < LANES - by, after, jnp.concatenate([after[1:], zero], axis=0))
        before = pltpu.roll(c, by, 2)
        before = jnp.where(lane < by, jnp.concatenate([zero, before[:-1]], axis=0), before)
        after_y = jnp.where(column == by - 1, 0.0, pltpu.roll(c, LANES - 1, 2))
        before_y = jnp.where(column == 0, 0.0, pltpu.roll(c, 1, 2))
        lam = rates[pl.ds(pl.multiple_of(d * SUB, SUB), SUB)]
        rb[d] = (sb[d] - lam[None] * c) - (4.0 * c - ((after + before) + (after_y + before_y)))

    loop(n, inner_remainder)

    def remainder(i):
        out_r[pl.ds(2 * tx * i, 2 * tx)] = backward(rb, i)

    loop(tiles // 2, remainder)

    for copy in late:
        copy.wait_recv()

    inner = pl.ds(PAD, by)
    out_r[0] += da[0, inner]
    out_r[bx - 1] += da[bx + 1, inner]

    def edges(i):
        sub = lax.broadcasted_iota(jnp.int32, (1, PAD, depth), 1)
        r = pl.ds(i, 1)
        first = pltpu.roll(da[pl.ds(1 + i, 1), 0:PAD], 1, 1)
        out_r[r, 0:PAD] += jnp.where(sub == 0, first, 0.0)
        last = pltpu.roll(da[pl.ds(1 + i, 1), PAD + by : 2 * PAD + by], PAD - 1, 1)
        out_r[r, by - PAD : by] += jnp.where(sub == PAD - 1, last, 0.0)

    loop(bx, edges)
    for copy in early + late:
        copy.wait_send()
    for end in ends:
        end()


def transform(depth, n):
    per = -(-depth // n)
    index = np.arange(1, depth + 1)
    angle = np.pi / (depth + 1)
    sines = np.sqrt(2.0 / (depth + 1)) * np.sin(angle * (np.outer(index, index) % (2 * (depth + 1))))
    rates = 4.0 * np.sin(0.5 * angle * index) ** 2
    matrix = np.zeros((n, SUB, depth))
    column = np.ones((n, SUB))
    for m in range(depth):
        matrix[m // per, m % per] = sines[m]
        column[m // per, m % per] = rates[m]
    rows = np.repeat(column.reshape(n * SUB, 1), LANES, axis=1)
    return matrix.reshape(n * SUB, depth).astype(np.float32), rows.astype(np.float32)


def on_device(nx, ny, forces, pressure_prev):
    bx, by, depth = pressure_prev.shape
    n = nx * ny
    f32 = jnp.float32
    width = ny * by
    tx = LANES // by
    tiles = bx // tx
    sine, rates = transform(depth, n)

    def vmem(*shape):
        return pltpu.VMEM(shape, f32)

    sem = pltpu.SemaphoreType.DMA
    padded = (bx + 2, by + 2 * PAD, depth)
    mail = (n, tiles, SUB, LANES)
    levels = []
    for level in range(LEVELS):
        count = 3 if level < LEVELS - 1 else 2
        levels += [vmem(nx * bx // 2**level + 2, SUB, width)] * count
    scratch = (
        [vmem(bx + 1, by, depth), vmem(bx, by + PAD, depth), vmem(bx, by, depth)]
        + [vmem(*padded)] * 2
        + [vmem(bx, by, depth), vmem(n * SUB, depth), vmem(n * SUB, LANES)]
        + [vmem(*mail)] * 4
        + levels
        + [sem((6,)), sem((2,)), sem((2,)), sem((2, 4)), sem((2, 4))]
        + [sem((n,))] * 4
    )
    shape = jax.ShapeDtypeStruct((bx, by, depth), f32)
    anyspace = pl.BlockSpec(memory_space=pl.ANY)
    vmemspace = pl.BlockSpec(memory_space=pltpu.VMEM)
    return pl.pallas_call(
        functools.partial(kernel, nx, ny),
        out_shape=(shape, shape),
        in_specs=[anyspace] * 4,
        out_specs=(vmemspace, vmemspace),
        scratch_shapes=scratch,
        compiler_params=pltpu.CompilerParams(
            collective_id=0, has_side_effects=True, vmem_limit_bytes=60 * 1024 * 1024
        ),
    )(forces, pressure_prev, sine, rates)


def solution(mesh):
    return jax.shard_map(
        functools.partial(on_device, mesh.shape["gx"], mesh.shape["gy"]),
        mesh=mesh,
        in_specs=(P(None, "gx", "gy", None), P("gx", "gy", None)),
        out_specs=(P("gx", "gy", None), P("gx", "gy", None)),
        check_vma=False,
    )
```

```python
import functools

import numpy as np

import jax
import jax.numpy as jnp
from jax import lax
from jax.experimental import pallas as pl
from jax.experimental.pallas import tpu as pltpu
from jax.sharding import PartitionSpec as P

OMEGA = 0.8
LEVELS = 5
CYCLES = 2
COARSE_SWEEPS = 4
SUB = 8
HALF = 4
LANES = 128
MESH = pl.DeviceIdType.MESH
EXACT = lax.Precision.HIGHEST


def loop(count, body):
    def step(i, carry):
        body(i)
        return carry

    lax.fori_loop(0, count, step, 0)


def low(shape):
    return lax.broadcasted_iota(jnp.int32, shape, len(shape) - 2) < HALF


def flip(c):
    return pltpu.roll(c, HALF, c.ndim - 2)


def swap(a, b):
    mask = low(a.shape)
    return jnp.where(mask, a, flip(b)), jnp.where(mask, flip(a), b)


def transposed(tiles, by):
    tiles = list(tiles)
    lane = lax.broadcasted_iota(jnp.int32, tiles[0].shape, tiles[0].ndim - 1)
    axis = tiles[0].ndim - 1
    step = 1
    while step < len(tiles):
        odd = (lane & (step * by)) != 0
        for g in range(len(tiles)):
            if g & step == 0:
                a, b = tiles[g], tiles[g + step]
                tiles[g] = jnp.where(odd, pltpu.roll(b, step * by, axis), a)
                tiles[g + step] = jnp.where(odd, b, pltpu.roll(a, LANES - step * by, axis))
        step *= 2
    return tiles


class Level:
    def __init__(self, index, rows, rate):
        self.rows, self.rate, self.shift = rows, rate, 2**index
        self.weight = 0.25**index
        self.k = OMEGA / (4.0 * self.weight + 2.0)
        self.unit = min(rows, 64 * LANES // rate.shape[1])

    def sides(self, c):
        axis = c.ndim - 1
        return pltpu.roll(c, self.shift, axis) + pltpu.roll(c, c.shape[axis] - self.shift, axis)

    def relax(self, c, lateral, f):
        keep = 1.0 - self.k * (4.0 * self.weight + self.rate)
        return keep * c + (self.k * self.weight) * lateral + self.k * f

    def begin(self, f, lateral):
        keep = self.k * (2.0 - self.k * (4.0 * self.weight + self.rate))
        return keep * f + (self.k * self.k * self.weight) * lateral

    def remainder(self, c, lateral, f):
        return (f - self.rate * c) - self.weight * (4.0 * c - lateral)

    def restrict(self, r):
        pairs = r.reshape((r.shape[0] // 2, 2) + r.shape[1:])
        s = pairs[:, 0] + pairs[:, 1]
        width = s.shape[2]
        lane = lax.broadcasted_iota(jnp.int32, s.shape, 2)
        odd = (lane & self.shift) != 0
        other = jnp.where(odd, pltpu.roll(s, self.shift, 2), pltpu.roll(s, width - self.shift, 2))
        return 0.25 * (s + other)

    def each(self, body):
        if self.unit == self.rows:
            body(0)
        else:
            loop(self.rows // self.unit, lambda i: body(pl.multiple_of(i * self.unit, self.unit)))

    def around(self, ref, x):
        block = ref[pl.ds(x, self.unit + 2)]
        c = block[1:-1]
        return c, (block[:-2] + block[2:]) + self.sides(c)

    def sweep(self, v, f, dst):
        def body(x):
            c, lateral = self.around(v, x)
            dst[pl.ds(1 + x, self.unit)] = self.relax(c, lateral, f[pl.ds(1 + x, self.unit)])

        self.each(body)
        ghosts(dst, self.rows)

    def sweep_twice_from_zero(self, f, dst):
        def body(x):
            c, lateral = self.around(f, x)
            dst[pl.ds(1 + x, self.unit)] = self.begin(c, lateral)

        self.each(body)
        ghosts(dst, self.rows)

    def restricted(self, v, f, dst):
        def body(x):
            c, lateral = self.around(v, x)
            r = self.remainder(c, lateral, f[pl.ds(1 + x, self.unit)])
            dst[pl.ds(1 + x // 2, self.unit // 2)] = self.restrict(r)

        self.each(body)
        ghosts(dst, self.rows // 2)

    def corrected_sweep(self, v, e, f, dst):
        def body(x):
            block = v[pl.ds(x, self.unit + 2)]
            half = e[pl.ds(x // 2, self.unit // 2 + 2)]
            pieces = [half[i] for i in range(self.unit // 2 + 2)]
            twice = [pieces[0]] + [p for p in pieces[1:-1] for _ in range(2)] + [pieces[-1]]
            block = block + jnp.stack(twice)
            c = block[1:-1]
            lateral = (block[:-2] + block[2:]) + self.sides(c)
            dst[pl.ds(1 + x, self.unit)] = self.relax(c, lateral, f[pl.ds(1 + x, self.unit)])

        self.each(body)
        ghosts(dst, self.rows)

    def solve(self, f):
        mean = jnp.sum(jnp.sum(f, axis=0), axis=1, keepdims=True)
        mean = (mean + flip(mean)) / (2 * self.rows * f.shape[2])
        v = jnp.broadcast_to((mean / self.rate)[None], f.shape)
        for _ in range(COARSE_SWEEPS):
            up = jnp.concatenate([flip(v[-1:]), v[:-1]], axis=0)
            down = jnp.concatenate([v[1:], flip(v[:1])], axis=0)
            v = self.relax(v, (up + down) + self.sides(v), f)
        return v


def ghosts(ref, rows):
    ref[0] = flip(ref[rows])
    ref[rows + 1] = flip(ref[1])


def kernel(
    nx, ny,
    forces, pressure, sine_in, decay_in, rates_in, out_p, out_r,
    fx, fy, fz, pa, da, g, sine, decay, rates, pre, sb, rb, sb2, rb2, ex, ey,
    f0, a0, b0, f1, a1, b1, f2, a2, b2, f3, a3, b3, f4, a4,
    local_sem, plane_send, plane_recv, halo_send, halo_recv,
    go_send, go_recv, back_send, back_recv,
):
    mx, my = lax.axis_index("gx"), lax.axis_index("gy")
    n = nx * ny
    me = mx * ny + my
    bx, by, depth = pressure.shape
    tx = LANES // by
    deep = bx // (2 * tx)
    cells = bx // 2 * by

    loads = [
        pltpu.make_async_copy(forces.at[0], fx.at[pl.ds(1, bx)], local_sem.at[0]),
        pltpu.make_async_copy(forces.at[1], fy, local_sem.at[1]),
        pltpu.make_async_copy(pressure, pa.at[pl.ds(1, bx)], local_sem.at[2]),
        pltpu.make_async_copy(forces.at[2], fz, local_sem.at[3]),
        pltpu.make_async_copy(sine_in, sine, local_sem.at[4]),
        pltpu.make_async_copy(decay_in, decay, local_sem.at[5]),
        pltpu.make_async_copy(rates_in, rates, local_sem.at[6]),
    ]
    for load in loads:
        load.start()

    def device(d):
        return d // ny, lax.rem(d, ny)

    barrier = pltpu.get_barrier_semaphore()

    def greet(j):
        pl.semaphore_signal(
            barrier, inc=1, device_id=device(lax.rem(me + 1 + j, n)), device_id_type=MESH
        )

    loop(n - 1, greet)
    fx[0] = jnp.zeros((by, depth), jnp.float32)
    pa[0] = jnp.zeros((by, depth), jnp.float32)
    pa[bx + 1] = jnp.zeros((by, depth), jnp.float32)
    for load in loads:
        load.wait()

    def make_source(i):
        r = 2 * i
        x = fx[pl.ds(r, 3)]
        y = fy[pl.ds(r, 2)]
        z = fz[pl.ds(r, 2)]
        p = pa[pl.ds(r, 4)]
        c = p[1:-1]
        lane = lax.broadcasted_iota(jnp.int32, z.shape, 2)
        column = lax.broadcasted_iota(jnp.int32, z.shape, 1)
        behind_z = jnp.where(lane == 0, 0.0, pltpu.roll(z, 1, 2))
        behind_y = jnp.where(column == 0, 0.0, pltpu.roll(y, 1, 1))
        source = (x[:-1] - x[1:]) + (behind_y - y) + (behind_z - z)
        before = jnp.where(column == 0, 0.0, pltpu.roll(c, 1, 1))
        after = jnp.where(column == by - 1, 0.0, pltpu.roll(c, by - 1, 1))
        around = (p[:-2] + p[2:]) + (before + after)
        g[pl.ds(r, 2)] = source - (4.0 * c - around)

    loop(bx // 2, make_source)

    def to_modes(matrix, rows):
        return lax.dot_general(
            matrix, rows.reshape(cells, depth), (((1,), (1,)), ((), ())),
            preferred_element_type=jnp.float32, precision=EXACT,
        )

    def prepare(q):
        h, c = q // 2, lax.rem(q, 2)
        pre[h, c] = to_modes(decay[h], pa[pl.ds(1 + c * (bx // 2), bx // 2)])

    loop(4, prepare)
    pl.semaphore_wait(barrier, n - 1)

    right, left = lax.rem(mx + 1, nx), lax.rem(mx + nx - 1, nx)
    above, below = lax.rem(my + 1, ny), lax.rem(my + ny - 1, ny)

    def remote(src, dst, send, recv, to):
        copy = pltpu.make_async_remote_copy(
            src_ref=src, dst_ref=dst, send_sem=send, recv_sem=recv,
            device_id=to, device_id_type=MESH,
        )
        copy.start()
        return copy

    rows = pl.ds(1, bx)

    def halo(ref, turn):
        def strip(d, src, dst, to):
            return remote(src, dst, halo_send.at[turn, d], halo_recv.at[turn, d], to)

        return [
            strip(0, ref.at[pl.ds(bx, 1)], ex.at[turn, pl.ds(0, 1)], (right, my)),
            strip(1, ref.at[pl.ds(1, 1)], ex.at[turn, pl.ds(1, 1)], (left, my)),
            strip(2, ref.at[rows, pl.ds(by - 1, 1)], ey.at[turn, :, pl.ds(0, 1)], (mx, above)),
            strip(3, ref.at[rows, pl.ds(0, 1)], ey.at[turn, :, pl.ds(SUB - 1, 1)], (mx, below)),
        ]

    def add_edges(ref, turn):
        ref[0] += ex[turn, 0]
        ref[bx - 1] += ex[turn, 1]
        sub = lax.broadcasted_iota(jnp.int32, (bx, SUB, depth), 1)
        ref[:, 0:SUB] += jnp.where(sub == 0, ey[turn], 0.0)
        ref[:, by - SUB : by] += jnp.where(sub == SUB - 1, ey[turn], 0.0)

    early = halo(pa, 0)
    early.append(
        remote(fx.at[pl.ds(bx, 1)], ex.at[2, pl.ds(0, 1)], plane_send.at[0], plane_recv.at[0], (right, my))
    )
    early.append(
        remote(
            fy.at[:, pl.ds(by - 1, 1)], ey.at[2, :, pl.ds(0, 1)],
            plane_send.at[1], plane_recv.at[1], (mx, above),
        )
    )
    for copy in early:
        copy.wait_recv()
    add_edges(g, 0)
    g[0] += ex[2, 0]
    column = lax.broadcasted_iota(jnp.int32, (bx, SUB, depth), 1)
    g[:, 0:SUB] += jnp.where(column == 0, ey[2], 0.0)

    class Exchange:
        def __init__(self, h, src, dst, send, recv):
            self.h, self.src, self.dst, self.send, self.recv = h, src, dst, send, recv

        def message(self, d, slot):
            h = self.h
            return pltpu.make_async_remote_copy(
                src_ref=self.src.at[h, d], dst_ref=self.dst.at[h, slot],
                send_sem=self.send.at[h, d], recv_sem=self.recv.at[h, slot],
                device_id=device(d), device_id_type=MESH,
            )

        def start(self):
            loop(n - 1, lambda j: self.message(lax.rem(me + 1 + j, n), me).start())
            self.dst[self.h, me] = self.src[self.h, me]

        def arrive(self):
            def one(j):
                d = lax.rem(me + n - 1 - j, n)
                self.message(d, d).wait_recv()

            loop(n - 1, one)

        def finish(self):
            def one(j):
                d = lax.rem(me + 1 + j, n)
                self.message(d, d).wait_send()

            loop(n - 1, one)

    def go(h):
        return Exchange(h, sb, rb, go_send, go_recv)

    def back(h):
        return Exchange(h, sb2, rb2, back_send, back_recv)

    def forward(h):
        modes = [to_modes(sine[h], g[pl.ds(c * (bx // 2), bx // 2)]) + pre[h, c] for c in range(2)]
        for p in range(deep):
            part = slice(p * LANES, (p + 1) * LANES)
            both = swap(*[m[:, part].reshape(n // 2, SUB, LANES) for m in modes])
            for parity in range(2):
                for e in range(n // 2):
                    sb[h, 2 * e + parity, p] = both[parity][e]
        go(h).start()

    loop(2, forward)

    def solve(h):
        go(h).arrive()
        for x in range(nx // 2):
            for p in range(deep):
                pairs = [swap(rb[h, x * ny + y, p], rb[h, (x + nx // 2) * ny + y, p]) for y in range(ny)]
                for c in range(2):
                    tiles = [pair[c] for pair in pairs]
                    groups = [transposed(tiles[k : k + tx], by) for k in range(0, ny, tx)]
                    first = 1 + x * bx + c * (bx // 2) + p * tx
                    for i in range(tx):
                        f0[first + i] = jnp.concatenate([group[i] for group in groups], axis=1)
        mine = rates[h, pl.ds(pl.multiple_of(me * SUB, SUB), SUB)]
        lam = jnp.concatenate([mine] * (ny * by // LANES), axis=1)
        count = nx * bx // 2
        l0, l1, l2, l3, l4 = (Level(i, count // 2**i, lam) for i in range(LEVELS))
        ghosts(f0, count)
        for cycle in range(CYCLES):
            if cycle == 0:
                l0.sweep_twice_from_zero(f0, a0)
            else:
                l0.sweep(a0, f0, b0)
                l0.sweep(b0, f0, a0)
            l0.restricted(a0, f0, f1)
            l1.sweep_twice_from_zero(f1, a1)
            l1.restricted(a1, f1, f2)
            l2.sweep_twice_from_zero(f2, a2)
            l2.restricted(a2, f2, f3)
            l3.sweep_twice_from_zero(f3, a3)
            l3.restricted(a3, f3, f4)
            a4[pl.ds(1, l4.rows)] = l4.solve(f4[pl.ds(1, l4.rows)])
            ghosts(a4, l4.rows)
            l3.corrected_sweep(a3, a4, f3, b3)
            l3.sweep(b3, f3, a3)
            l2.corrected_sweep(a2, a3, f2, b2)
            l2.sweep(b2, f2, a2)
            l1.corrected_sweep(a1, a2, f1, b1)
            l1.sweep(b1, f1, a1)
            l0.corrected_sweep(a0, a1, f0, b0)
            l0.sweep(b0, f0, a0)
        for x in range(nx // 2):
            for p in range(deep):
                kept = []
                for c in range(2):
                    first = 1 + x * bx + c * (bx // 2) + p * tx
                    block = a0[pl.ds(first, tx)]
                    tiles = []
                    for k in range(ny // tx):
                        part = slice(k * LANES, (k + 1) * LANES)
                        tiles += transposed([block[i][:, part] for i in range(tx)], by)
                    kept.append(tiles)
                for y in range(ny):
                    one, other = swap(kept[0][y], kept[1][y])
                    sb2[h, x * ny + y, p] = one
                    sb2[h, (x + nx // 2) * ny + y, p] = other
        back(h).start()

    loop(2, solve)

    def to_cells(mail, h):
        parts = [[], []]
        for p in range(deep):
            tiles = [
                swap(mail[h, 2 * e, p], mail[h, 2 * e + 1, p]) for e in range(n // 2)
            ]
            for c in range(2):
                parts[c].append(jnp.concatenate([t[c] for t in tiles], axis=0))
        for c in range(2):
            values = lax.dot_general(
                jnp.concatenate(parts[c], axis=1), sine[h], (((0,), (0,)), ((), ())),
                preferred_element_type=jnp.float32, precision=EXACT,
            )
            yield c * (bx // 2), values.reshape(bx // 2, by, depth)

    def inner_remainder(h, d):
        c = rb2[h, d]
        lane = lax.broadcasted_iota(jnp.int32, c.shape, 2)
        lower = low((1, SUB, LANES))
        column = lax.rem(lane, by)
        after = pltpu.roll(c, LANES - by, 2)
        beyond = jnp.where(lower, flip(after[:1]), 0.0)
        after = jnp.where(lane < LANES - by, after, jnp.concatenate([after[1:], beyond], axis=0))
        before = pltpu.roll(c, by, 2)
        beyond = jnp.where(lower, 0.0, flip(before[-1:]))
        before = jnp.where(lane < by, jnp.concatenate([beyond, before[:-1]], axis=0), before)
        after_y = jnp.where(column == by - 1, 0.0, pltpu.roll(c, LANES - 1, 2))
        before_y = jnp.where(column == 0, 0.0, pltpu.roll(c, 1, 2))
        lam = rates[h, pl.ds(pl.multiple_of(d * SUB, SUB), SUB)][None]
        rb[h, d] = (sb[h, d] - lam * c) - (4.0 * c - ((after + before) + (after_y + before_y)))

    def remainders(h):
        def several(i):
            for j in range(8):
                inner_remainder(h, 8 * i + j)

        loop(n // 8, several)

    half = bx // 2
    back(0).arrive()
    for r, values in to_cells(rb2, 0):
        da[pl.ds(1 + r, half)] = values
    remainders(0)
    for r, values in to_cells(rb, 0):
        out_r[pl.ds(r, half)] = values
    back(1).arrive()
    for r, values in to_cells(rb2, 1):
        da[pl.ds(1 + r, half)] += values
    late = halo(da, 1)
    remainders(1)
    for r, values in to_cells(rb, 1):
        out_r[pl.ds(r, half)] += values
    out_p[...] = pa[pl.ds(1, bx)] + da[pl.ds(1, bx)]
    for copy in late:
        copy.wait_recv()
    add_edges(out_r, 1)
    for copy in early + late:
        copy.wait_send()
    for h in range(2):
        go(h).finish()
        back(h).finish()


def transform(depth, n):
    per = -(-depth // n)
    each = -(-per // 2)
    index = np.arange(1, depth + 1)
    angle = np.pi / (depth + 1)
    sines = np.sqrt(2.0 / (depth + 1)) * np.sin(angle * (np.outer(index, index) % (2 * (depth + 1))))
    rates = 4.0 * np.sin(0.5 * angle * index) ** 2
    matrix = np.zeros((2, n, HALF, depth))
    column = np.ones((2, n, 2, HALF))
    decay = np.zeros((2, n, HALF, depth))
    for m in range(depth):
        d, h, j = m // per, m % per // each, m % per % each
        matrix[h, d, j] = sines[m]
        decay[h, d, j] = -rates[m] * sines[m]
        column[h, d, :, j] = rates[m]
    column = np.repeat(column.reshape(2, n * SUB, 1), LANES, axis=2)
    arrays = matrix.reshape(2, n * HALF, depth), decay.reshape(2, n * HALF, depth), column
    return [a.astype(np.float32) for a in arrays]


def on_device(nx, ny, forces, pressure_prev):
    bx, by, depth = pressure_prev.shape
    n = nx * ny
    f32 = jnp.float32
    width = ny * by
    tx = LANES // by
    deep = bx // (2 * tx)
    constants = transform(depth, n)

    def vmem(*shape):
        return pltpu.VMEM(shape, f32)

    sem = pltpu.SemaphoreType.DMA
    block = (bx, by, depth)
    levels = []
    for level in range(LEVELS):
        count = 3 if level < LEVELS - 1 else 2
        levels += [vmem(nx * bx // 2 // 2**level + 2, SUB, width)] * count
    scratch = (
        [vmem(bx + 1, by, depth), vmem(*block), vmem(*block)]
        + [vmem(bx + 2, by, depth)] * 2
        + [vmem(*block)]
        + [vmem(*c.shape) for c in constants]
        + [vmem(2, 2, n * HALF, bx // 2 * by)]
        + [vmem(2, n, deep, SUB, LANES)] * 4
        + [vmem(3, 2, by, depth), vmem(3, bx, SUB, depth)]
        + levels
        + [sem((7,)), sem((2,)), sem((2,)), sem((2, 4)), sem((2, 4))]
        + [sem((2, n))] * 4
    )
    shape = jax.ShapeDtypeStruct(block, f32)
    anyspace = pl.BlockSpec(memory_space=pl.ANY)
    vmemspace = pl.BlockSpec(memory_space=pltpu.VMEM)
    return pl.pallas_call(
        functools.partial(kernel, nx, ny),
        out_shape=(shape, shape),
        in_specs=[anyspace] * 5,
        out_specs=(vmemspace, vmemspace),
        scratch_shapes=scratch,
        compiler_params=pltpu.CompilerParams(
            collective_id=0, has_side_effects=True, vmem_limit_bytes=60 * 1024 * 1024
        ),
    )(forces, pressure_prev, *constants)


def solution(mesh):
    return jax.shard_map(
        functools.partial(on_device, mesh.shape["gx"], mesh.shape["gy"]),
        mesh=mesh,
        in_specs=(P(None, "gx", "gy", None), P("gx", "gy", None)),
        out_specs=(P("gx", "gy", None), P("gx", "gy", None)),
        check_vma=False,
    )
```

```python
import functools

import numpy as np

import jax
import jax.numpy as jnp
from jax import lax
from jax.experimental import pallas as pl
from jax.experimental.pallas import tpu as pltpu
from jax.sharding import PartitionSpec as P

OMEGA = 0.8
LEVELS = 5
CYCLES = 2
COARSE_SWEEPS = 4
SUB = 8
HALF = 4
LANES = 128
MESH = pl.DeviceIdType.MESH
EXACT = lax.Precision.HIGHEST


def loop(count, body):
    def step(i, carry):
        body(i)
        return carry

    lax.fori_loop(0, count, step, 0)


def low(shape):
    return lax.broadcasted_iota(jnp.int32, shape, len(shape) - 2) < HALF


def flip(c):
    return pltpu.roll(c, HALF, c.ndim - 2)


def swap(a, b):
    mask = low(a.shape)
    return jnp.where(mask, a, flip(b)), jnp.where(mask, flip(a), b)


def transposed(tiles, by):
    tiles = list(tiles)
    lane = lax.broadcasted_iota(jnp.int32, tiles[0].shape, tiles[0].ndim - 1)
    axis = tiles[0].ndim - 1
    step = 1
    while step < len(tiles):
        odd = (lane & (step * by)) != 0
        for g in range(len(tiles)):
            if g & step == 0:
                a, b = tiles[g], tiles[g + step]
                tiles[g] = jnp.where(odd, pltpu.roll(b, step * by, axis), a)
                tiles[g + step] = jnp.where(odd, b, pltpu.roll(a, LANES - step * by, axis))
        step *= 2
    return tiles


class Level:
    def __init__(self, index, rows, rate, waves):
        self.rows, self.rate = rows, rate
        self.width = rate.shape[1]
        self.period = self.width // 2**index
        self.weight = 0.25**index
        self.k = OMEGA / (4.0 * self.weight + 2.0)
        self.unit = min(rows, 64 * LANES // self.width)
        self.side, self.pair = (waves[i, pl.ds(index * SUB, SUB)] for i in range(2))

    def symbol(self):
        return self.k * (self.weight * self.side + self.rate)

    def relax(self, c, beside, f):
        return (1.0 - self.symbol()) * c + (self.k * self.weight) * beside + self.k * f

    def begin(self, f, beside):
        return (self.k * (2.0 - self.symbol())) * f + (self.k * self.k * self.weight) * beside

    def remainder(self, c, beside, f):
        return (f - self.rate * c) - self.weight * (self.side * c - beside)

    def restrict(self, r):
        pairs = r.reshape((r.shape[0] // 2, 2) + r.shape[1:])
        s = (0.5 * self.pair) * (pairs[:, 0] + pairs[:, 1])
        return s + pltpu.roll(s, self.period // 2, 2)

    def each(self, body):
        if self.unit == self.rows:
            body(0)
        else:
            loop(self.rows // self.unit, lambda i: body(pl.multiple_of(i * self.unit, self.unit)))

    def around(self, ref, x):
        block = ref[pl.ds(x, self.unit + 2)]
        return block[1:-1], block[:-2] + block[2:]

    def sweep(self, v, f, dst):
        def body(x):
            c, beside = self.around(v, x)
            dst[pl.ds(1 + x, self.unit)] = self.relax(c, beside, f[pl.ds(1 + x, self.unit)])

        self.each(body)
        ghosts(dst, self.rows)

    def sweep_twice_from_zero(self, f, dst):
        def body(x):
            c, beside = self.around(f, x)
            dst[pl.ds(1 + x, self.unit)] = self.begin(c, beside)

        self.each(body)
        ghosts(dst, self.rows)

    def restricted(self, v, f, dst):
        def body(x):
            c, beside = self.around(v, x)
            r = self.remainder(c, beside, f[pl.ds(1 + x, self.unit)])
            dst[pl.ds(1 + x // 2, self.unit // 2)] = self.restrict(r)

        self.each(body)
        ghosts(dst, self.rows // 2)

    def corrected_sweep(self, v, e, f, dst):
        def body(x):
            block = v[pl.ds(x, self.unit + 2)]
            half = self.pair * e[pl.ds(x // 2, self.unit // 2 + 2)]
            pieces = [half[i] for i in range(self.unit // 2 + 2)]
            twice = [pieces[0]] + [p for p in pieces[1:-1] for _ in range(2)] + [pieces[-1]]
            block = block + jnp.stack(twice)
            c, beside = block[1:-1], block[:-2] + block[2:]
            dst[pl.ds(1 + x, self.unit)] = self.relax(c, beside, f[pl.ds(1 + x, self.unit)])

        self.each(body)
        ghosts(dst, self.rows)

    def solve(self, f):
        mean = jnp.sum(f, axis=0)
        mean = (mean + flip(mean)) / (2 * self.rows)
        lane = lax.broadcasted_iota(jnp.int32, mean.shape, 1)
        mean = jnp.where(lax.rem(lane, self.period) == 0, mean / self.rate, 0.0)
        v = jnp.broadcast_to(mean[None], f.shape)
        for _ in range(COARSE_SWEEPS):
            up = jnp.concatenate([flip(v[-1:]), v[:-1]], axis=0)
            down = jnp.concatenate([v[1:], flip(v[:1])], axis=0)
            v = self.relax(v, up + down, f)
        return v


def ghosts(ref, rows):
    ref[0] = flip(ref[rows])
    ref[rows + 1] = flip(ref[1])


def kernel(
    nx, ny,
    forces, pressure, tables, out_p, out_r,
    fx, fy, fz, pa, da, g, sine, decay, rates, hartley, waves, pre, sb, rb, sb2, rb2, ex, ey,
    f0, a0, b0, f1, a1, b1, f2, a2, b2, f3, a3, b3, f4, a4,
    local_sem, plane_send, plane_recv, halo_send, halo_recv,
    go_send, go_recv, back_send, back_recv,
):
    mx, my = lax.axis_index("gx"), lax.axis_index("gy")
    n = nx * ny
    me = mx * ny + my
    bx, by, depth = pressure.shape
    tx = LANES // by
    deep = bx // (2 * tx)
    cells = bx // 2 * by

    loads = [
        pltpu.make_async_copy(forces.at[0], fx.at[pl.ds(1, bx)], local_sem.at[0]),
        pltpu.make_async_copy(forces.at[1], fy, local_sem.at[1]),
        pltpu.make_async_copy(pressure, pa.at[pl.ds(1, bx)], local_sem.at[2]),
        pltpu.make_async_copy(forces.at[2], fz, local_sem.at[3]),
    ]
    at = 0
    for ref in (sine, decay, rates, hartley, waves):
        for h in range(2):
            count, width = ref.shape[1:]
            part = tables.at[pl.ds(at, count), pl.ds(0, width)]
            loads.append(pltpu.make_async_copy(part, ref.at[h], local_sem.at[len(loads)]))
            at += count
    for load in loads:
        load.start()

    def device(d):
        return d // ny, lax.rem(d, ny)

    barrier = pltpu.get_barrier_semaphore()

    def greet(j):
        pl.semaphore_signal(
            barrier, inc=1, device_id=device(lax.rem(me + 1 + j, n)), device_id_type=MESH
        )

    loop(n - 1, greet)
    fx[0] = jnp.zeros((by, depth), jnp.float32)
    pa[0] = jnp.zeros((by, depth), jnp.float32)
    pa[bx + 1] = jnp.zeros((by, depth), jnp.float32)
    for load in loads[:3]:
        load.wait()
    pl.semaphore_wait(barrier, n - 1)

    right, left = lax.rem(mx + 1, nx), lax.rem(mx + nx - 1, nx)
    above, below = lax.rem(my + 1, ny), lax.rem(my + ny - 1, ny)

    def remote(src, dst, send, recv, to):
        copy = pltpu.make_async_remote_copy(
            src_ref=src, dst_ref=dst, send_sem=send, recv_sem=recv,
            device_id=to, device_id_type=MESH,
        )
        copy.start()
        return copy

    rows = pl.ds(1, bx)

    def halo(ref, turn):
        def strip(d, src, dst, to):
            return remote(src, dst, halo_send.at[turn, d], halo_recv.at[turn, d], to)

        return [
            strip(0, ref.at[pl.ds(bx, 1)], ex.at[turn, pl.ds(0, 1)], (right, my)),
            strip(1, ref.at[pl.ds(1, 1)], ex.at[turn, pl.ds(1, 1)], (left, my)),
            strip(2, ref.at[rows, pl.ds(by - 1, 1)], ey.at[turn, :, pl.ds(0, 1)], (mx, above)),
            strip(3, ref.at[rows, pl.ds(0, 1)], ey.at[turn, :, pl.ds(SUB - 1, 1)], (mx, below)),
        ]

    def add_edges(ref, turn):
        ref[0] += ex[turn, 0]
        ref[bx - 1] += ex[turn, 1]
        sub = lax.broadcasted_iota(jnp.int32, (bx, SUB, depth), 1)
        ref[:, 0:SUB] += jnp.where(sub == 0, ey[turn], 0.0)
        ref[:, by - SUB : by] += jnp.where(sub == SUB - 1, ey[turn], 0.0)

    early = halo(pa, 0)
    early.append(
        remote(fx.at[pl.ds(bx, 1)], ex.at[2, pl.ds(0, 1)], plane_send.at[0], plane_recv.at[0], (right, my))
    )
    early.append(
        remote(
            fy.at[:, pl.ds(by - 1, 1)], ey.at[2, :, pl.ds(0, 1)],
            plane_send.at[1], plane_recv.at[1], (mx, above),
        )
    )
    for load in loads[3:]:
        load.wait()

    def make_source(i):
        r = 2 * i
        x = fx[pl.ds(r, 3)]
        y = fy[pl.ds(r, 2)]
        z = fz[pl.ds(r, 2)]
        p = pa[pl.ds(r, 4)]
        c = p[1:-1]
        lane = lax.broadcasted_iota(jnp.int32, z.shape, 2)
        column = lax.broadcasted_iota(jnp.int32, z.shape, 1)
        behind_z = jnp.where(lane == 0, 0.0, pltpu.roll(z, 1, 2))
        behind_y = jnp.where(column == 0, 0.0, pltpu.roll(y, 1, 1))
        source = (x[:-1] - x[1:]) + (behind_y - y) + (behind_z - z)
        before = jnp.where(column == 0, 0.0, pltpu.roll(c, 1, 1))
        after = jnp.where(column == by - 1, 0.0, pltpu.roll(c, by - 1, 1))
        around = (p[:-2] + p[2:]) + (before + after)
        g[pl.ds(r, 2)] = source - (4.0 * c - around)

    loop(bx // 2, make_source)

    def to_modes(matrix, rows):
        return lax.dot_general(
            matrix, rows.reshape(cells, depth), (((1,), (1,)), ((), ())),
            preferred_element_type=jnp.float32, precision=EXACT,
        )

    def prepare(q):
        h, c = q // 2, lax.rem(q, 2)
        pre[h, c] = to_modes(decay[h], pa[pl.ds(1 + c * (bx // 2), bx // 2)])

    loop(4, prepare)
    for copy in early:
        copy.wait_recv()
    add_edges(g, 0)
    g[0] += ex[2, 0]
    column = lax.broadcasted_iota(jnp.int32, (bx, SUB, depth), 1)
    g[:, 0:SUB] += jnp.where(column == 0, ey[2], 0.0)

    class Exchange:
        def __init__(self, h, src, dst, send, recv):
            self.h, self.src, self.dst, self.send, self.recv = h, src, dst, send, recv

        def copy(self, src, dst, to):
            return pltpu.make_async_remote_copy(
                src_ref=src, dst_ref=dst, send_sem=self.send.at[self.h], recv_sem=self.recv.at[self.h],
                device_id=to, device_id_type=MESH,
            )

        def start(self):
            src, dst = self.src.at[self.h], self.dst.at[self.h]

            def column(i, first):
                x = mx + i
                x = jnp.where(x >= nx, x - nx, x)
                for j in range(first, ny):
                    y = my + j
                    y = jnp.where(y >= ny, y - ny, y)
                    self.copy(src.at[x * ny + y], dst.at[me], (x, y)).start()

            loop(nx - 1, lambda i: column(i + 1, 0))
            column(0, 1)
            self.dst[self.h, me] = self.src[self.h, me]

        def all(self):
            most = pl.ds(0, n - 1)
            return self.copy(self.src.at[self.h, most], self.dst.at[self.h, most], (left, my))

        def arrive(self):
            self.all().wait_recv()

        def finish(self):
            self.all().wait_send()

    def go(h):
        return Exchange(h, sb, rb, go_send, go_recv)

    def back(h):
        return Exchange(h, sb2, rb2, back_send, back_recv)

    def forward(h):
        modes = [to_modes(sine[h], g[pl.ds(c * (bx // 2), bx // 2)]) + pre[h, c] for c in range(2)]
        for p in range(deep):
            part = slice(p * LANES, (p + 1) * LANES)
            both = swap(*[m[:, part].reshape(n // 2, SUB, LANES) for m in modes])
            for parity in range(2):
                for e in range(n // 2):
                    sb[h, 2 * e + parity, p] = both[parity][e]
        go(h).start()

    loop(2, forward)

    def solve(h):
        go(h).arrive()
        for x in range(nx // 2):
            for p in range(deep):
                pairs = [swap(rb[h, x * ny + y, p], rb[h, (x + nx // 2) * ny + y, p]) for y in range(ny)]
                for c in range(2):
                    tiles = [pair[c] for pair in pairs]
                    groups = [transposed(tiles[k : k + tx], by) for k in range(0, ny, tx)]
                    first = 1 + x * bx + c * (bx // 2) + p * tx
                    for i in range(tx):
                        f0[first + i] = jnp.concatenate([group[i] for group in groups], axis=1)
        mine = rates[h, pl.ds(pl.multiple_of(me * SUB, SUB), SUB)]
        lam = jnp.concatenate([mine] * (ny * by // LANES), axis=1)
        count = nx * bx // 2
        l0, l1, l2, l3, l4 = (Level(i, count // 2**i, lam, waves) for i in range(LEVELS))
        inner = pl.ds(1, count)

        def along_y(ref, direction):
            return lax.dot_general(
                ref[inner].reshape(count * SUB, ny * by), hartley[direction], (((1,), (0,)), ((), ())),
                preferred_element_type=jnp.float32, precision=EXACT,
            ).reshape(count, SUB, ny * by)

        f0[inner] = along_y(f0, 0)
        ghosts(f0, count)
        for cycle in range(CYCLES):
            if cycle == 0:
                l0.sweep_twice_from_zero(f0, a0)
            else:
                l0.sweep(a0, f0, b0)
                l0.sweep(b0, f0, a0)
            l0.restricted(a0, f0, f1)
            l1.sweep_twice_from_zero(f1, a1)
            l1.restricted(a1, f1, f2)
            l2.sweep_twice_from_zero(f2, a2)
            l2.restricted(a2, f2, f3)
            l3.sweep_twice_from_zero(f3, a3)
            l3.restricted(a3, f3, f4)
            a4[pl.ds(1, l4.rows)] = l4.solve(f4[pl.ds(1, l4.rows)])
            ghosts(a4, l4.rows)
            l3.corrected_sweep(a3, a4, f3, b3)
            l3.sweep(b3, f3, a3)
            l2.corrected_sweep(a2, a3, f2, b2)
            l2.sweep(b2, f2, a2)
            l1.corrected_sweep(a1, a2, f1, b1)
            l1.sweep(b1, f1, a1)
            l0.corrected_sweep(a0, a1, f0, b0)
            l0.sweep(b0, f0, a0)
        b0[inner] = along_y(a0, 1)
        for x in range(nx // 2):
            for p in range(deep):
                kept = []
                for c in range(2):
                    first = 1 + x * bx + c * (bx // 2) + p * tx
                    block = b0[pl.ds(first, tx)]
                    tiles = []
                    for k in range(ny // tx):
                        part = slice(k * LANES, (k + 1) * LANES)
                        tiles += transposed([block[i][:, part] for i in range(tx)], by)
                    kept.append(tiles)
                for y in range(ny):
                    one, other = swap(kept[0][y], kept[1][y])
                    sb2[h, x * ny + y, p] = one
                    sb2[h, (x + nx // 2) * ny + y, p] = other
        back(h).start()

    loop(2, solve)

    def to_cells(mail, h):
        parts = [[], []]
        for p in range(deep):
            tiles = [
                swap(mail[h, 2 * e, p], mail[h, 2 * e + 1, p]) for e in range(n // 2)
            ]
            for c in range(2):
                parts[c].append(jnp.concatenate([t[c] for t in tiles], axis=0))
        for c in range(2):
            values = lax.dot_general(
                jnp.concatenate(parts[c], axis=1), sine[h], (((0,), (0,)), ((), ())),
                preferred_element_type=jnp.float32, precision=EXACT,
            )
            yield c * (bx // 2), values.reshape(bx // 2, by, depth)

    def inner_remainder(h, d):
        c = rb2[h, d]
        lane = lax.broadcasted_iota(jnp.int32, c.shape, 2)
        lower = low((1, SUB, LANES))
        column = lax.rem(lane, by)
        after = pltpu.roll(c, LANES - by, 2)
        beyond = jnp.where(lower, flip(after[:1]), 0.0)
        after = jnp.where(lane < LANES - by, after, jnp.concatenate([after[1:], beyond], axis=0))
        before = pltpu.roll(c, by, 2)
        beyond = jnp.where(lower, 0.0, flip(before[-1:]))
        before = jnp.where(lane < by, jnp.concatenate([beyond, before[:-1]], axis=0), before)
        after_y = jnp.where(column == by - 1, 0.0, pltpu.roll(c, LANES - 1, 2))
        before_y = jnp.where(column == 0, 0.0, pltpu.roll(c, 1, 2))
        lam = rates[h, pl.ds(pl.multiple_of(d * SUB, SUB), SUB)][None]
        rb[h, d] = (sb[h, d] - lam * c) - (4.0 * c - ((after + before) + (after_y + before_y)))

    def remainders(h):
        def several(i):
            for j in range(8):
                inner_remainder(h, 8 * i + j)

        loop(n // 8, several)

    half = bx // 2
    back(0).arrive()
    for r, values in to_cells(rb2, 0):
        da[pl.ds(1 + r, half)] = values
    remainders(0)
    for r, values in to_cells(rb, 0):
        out_r[pl.ds(r, half)] = values
    back(1).arrive()
    for r, values in to_cells(rb2, 1):
        da[pl.ds(1 + r, half)] += values
    late = halo(da, 1)
    remainders(1)
    for r, values in to_cells(rb, 1):
        out_r[pl.ds(r, half)] += values
    out_p[...] = pa[pl.ds(1, bx)] + da[pl.ds(1, bx)]
    for copy in late:
        copy.wait_recv()
    add_edges(out_r, 1)
    for copy in early + late:
        copy.wait_send()
    for h in range(2):
        go(h).finish()
        back(h).finish()


def transform(depth, n, width):
    per = -(-depth // n)
    each = -(-per // 2)
    index = np.arange(1, depth + 1)
    angle = np.pi / (depth + 1)
    sines = np.sqrt(2.0 / (depth + 1)) * np.sin(angle * (np.outer(index, index) % (2 * (depth + 1))))
    rates = 4.0 * np.sin(0.5 * angle * index) ** 2
    matrix = np.zeros((2, n, HALF, depth))
    column = np.ones((2, n, 2, HALF))
    decay = np.zeros((2, n, HALF, depth))
    for m in range(depth):
        d, h, j = m // per, m % per // each, m % per % each
        matrix[h, d, j] = sines[m]
        decay[h, d, j] = -rates[m] * sines[m]
        column[h, d, :, j] = rates[m]
    column = np.repeat(column.reshape(2, n * SUB, 1), LANES, axis=2)
    angle = 2 * np.pi / (2 * width) * (np.outer(np.arange(width), 2 * np.arange(width) + 1) % (2 * width))
    cas = np.cos(angle) + np.sin(angle)
    waves = np.zeros((2, LEVELS, SUB, width))
    for level in range(LEVELS):
        period = width // 2**level
        q = np.arange(width) % period
        waves[0, level] = 4.0 - 2.0 * np.cos(2 * np.pi * q / period)
        waves[1, level] = np.cos(np.pi * q / period) * np.where(2 * q < period, 1.0, -1.0)
    hartley = np.stack([cas.T / width, cas])
    return [
        matrix.reshape(2, n * HALF, depth), decay.reshape(2, n * HALF, depth), column,
        hartley, waves.reshape(2, LEVELS * SUB, width),
    ]


def stacked(arrays):
    wide = max(a.shape[2] for a in arrays)
    padded = [np.pad(a, ((0, 0), (0, 0), (0, wide - a.shape[2]))) for a in arrays]
    return np.concatenate([half for a in padded for half in a]).astype(np.float32)


def on_device(nx, ny, forces, pressure_prev):
    bx, by, depth = pressure_prev.shape
    n = nx * ny
    f32 = jnp.float32
    width = ny * by
    tx = LANES // by
    deep = bx // (2 * tx)
    constants = transform(depth, n, width)

    def vmem(*shape):
        return pltpu.VMEM(shape, f32)

    sem = pltpu.SemaphoreType.DMA
    block = (bx, by, depth)
    levels = []
    for level in range(LEVELS):
        count = 3 if level < LEVELS - 1 else 2
        levels += [vmem(nx * bx // 2 // 2**level + 2, SUB, width)] * count
    scratch = (
        [vmem(bx + 1, by, depth), vmem(*block), vmem(*block)]
        + [vmem(bx + 2, by, depth)] * 2
        + [vmem(*block)]
        + [vmem(*c.shape) for c in constants]
        + [vmem(2, 2, n * HALF, bx // 2 * by)]
        + [vmem(2, n, deep, SUB, LANES)] * 4
        + [vmem(3, 2, by, depth), vmem(3, bx, SUB, depth)]
        + levels
        + [sem((14,)), sem((2,)), sem((2,)), sem((2, 4)), sem((2, 4))]
        + [sem((2,))] * 4
    )
    shape = jax.ShapeDtypeStruct(block, f32)
    hbmspace = pl.BlockSpec(memory_space=pltpu.HBM)
    vmemspace = pl.BlockSpec(memory_space=pltpu.VMEM)
    return pl.pallas_call(
        functools.partial(kernel, nx, ny),
        out_shape=(shape, shape),
        in_specs=[hbmspace] * 3,
        out_specs=(vmemspace, vmemspace),
        scratch_shapes=scratch,
        compiler_params=pltpu.CompilerParams(
            collective_id=0, has_side_effects=True, vmem_limit_bytes=67043328 - int(11.2 * 1024 * 1024)
        ),
    )(forces, pressure_prev, stacked(constants))


def solution(mesh):
    return jax.shard_map(
        functools.partial(on_device, mesh.shape["gx"], mesh.shape["gy"]),
        mesh=mesh,
        in_specs=(P(None, "gx", "gy", None), P("gx", "gy", None)),
        out_specs=(P("gx", "gy", None), P("gx", "gy", None)),
        check_vma=False,
    )
```

```python
import functools

import numpy as np

import jax
import jax.numpy as jnp
from jax import lax
from jax.experimental import pallas as pl
from jax.experimental.pallas import tpu as pltpu
from jax.sharding import PartitionSpec as P

OMEGA = 0.8
LEVELS = 5
CYCLES = 2
COARSE_SWEEPS = 4
SUB = 8
HALF = 4
LANES = 128
MESH = pl.DeviceIdType.MESH
EXACT = lax.Precision.HIGHEST


def loop(count, body):
    def step(i, carry):
        body(i)
        return carry

    lax.fori_loop(0, count, step, 0)


def low(shape):
    return lax.broadcasted_iota(jnp.int32, shape, len(shape) - 2) < HALF


def flip(c):
    return pltpu.roll(c, HALF, c.ndim - 2)


def swap(a, b):
    mask = low(a.shape)
    return jnp.where(mask, a, flip(b)), jnp.where(mask, flip(a), b)


def transposed(tiles, by):
    tiles = list(tiles)
    lane = lax.broadcasted_iota(jnp.int32, tiles[0].shape, tiles[0].ndim - 1)
    axis = tiles[0].ndim - 1
    step = 1
    while step < len(tiles):
        odd = (lane & (step * by)) != 0
        for g in range(len(tiles)):
            if g & step == 0:
                a, b = tiles[g], tiles[g + step]
                tiles[g] = jnp.where(odd, pltpu.roll(b, step * by, axis), a)
                tiles[g + step] = jnp.where(odd, b, pltpu.roll(a, LANES - step * by, axis))
        step *= 2
    return tiles


def tile(mail, h, d, p):
    return mail[h, d, pl.ds(p * SUB, SUB)]


class Level:
    def __init__(self, index, rows, rate, waves):
        self.rows, self.rate = rows, rate
        self.width = rate.shape[1]
        self.period = self.width // 2**index
        self.weight = 0.25**index
        self.k = OMEGA / (4.0 * self.weight + 2.0)
        self.unit = min(rows, 64 * LANES // self.width)
        self.side, self.pair = (waves[i, pl.ds(index * SUB, SUB)] for i in range(2))

    def symbol(self):
        return self.k * (self.weight * self.side + self.rate)

    def relax(self, c, beside, f):
        return (1.0 - self.symbol()) * c + (self.k * self.weight) * beside + self.k * f

    def begin(self, f, beside):
        return (self.k * (2.0 - self.symbol())) * f + (self.k * self.k * self.weight) * beside

    def remainder(self, c, beside, f):
        return (f - self.rate * c) - self.weight * (self.side * c - beside)

    def restrict(self, r):
        pairs = r.reshape((r.shape[0] // 2, 2) + r.shape[1:])
        s = (0.5 * self.pair) * (pairs[:, 0] + pairs[:, 1])
        return s + pltpu.roll(s, self.period // 2, 2)

    def each(self, body):
        if self.unit == self.rows:
            body(0)
        else:
            loop(self.rows // self.unit, lambda i: body(pl.multiple_of(i * self.unit, self.unit)))

    def around(self, ref, x):
        block = ref[pl.ds(x, self.unit + 2)]
        return block[1:-1], block[:-2] + block[2:]

    def sweep(self, v, f, dst):
        def body(x):
            c, beside = self.around(v, x)
            dst[pl.ds(1 + x, self.unit)] = self.relax(c, beside, f[pl.ds(1 + x, self.unit)])

        self.each(body)
        ghosts(dst, self.rows)

    def sweep_twice_from_zero(self, f, dst):
        def body(x):
            c, beside = self.around(f, x)
            dst[pl.ds(1 + x, self.unit)] = self.begin(c, beside)

        self.each(body)
        ghosts(dst, self.rows)

    def restricted(self, v, f, dst):
        def body(x):
            c, beside = self.around(v, x)
            r = self.remainder(c, beside, f[pl.ds(1 + x, self.unit)])
            dst[pl.ds(1 + x // 2, self.unit // 2)] = self.restrict(r)

        self.each(body)
        ghosts(dst, self.rows // 2)

    def corrected_sweep(self, v, e, f, dst):
        def body(x):
            block = v[pl.ds(x, self.unit + 2)]
            half = self.pair * e[pl.ds(x // 2, self.unit // 2 + 2)]
            pieces = [half[i] for i in range(self.unit // 2 + 2)]
            twice = [pieces[0]] + [p for p in pieces[1:-1] for _ in range(2)] + [pieces[-1]]
            block = block + jnp.stack(twice)
            c, beside = block[1:-1], block[:-2] + block[2:]
            dst[pl.ds(1 + x, self.unit)] = self.relax(c, beside, f[pl.ds(1 + x, self.unit)])

        self.each(body)
        ghosts(dst, self.rows)

    def solve(self, f):
        mean = jnp.sum(f, axis=0)
        mean = (mean + flip(mean)) / (2 * self.rows)
        lane = lax.broadcasted_iota(jnp.int32, mean.shape, 1)
        mean = jnp.where(lax.rem(lane, self.period) == 0, mean / self.rate, 0.0)
        v = jnp.broadcast_to(mean[None], f.shape)
        for _ in range(COARSE_SWEEPS):
            up = jnp.concatenate([flip(v[-1:]), v[:-1]], axis=0)
            down = jnp.concatenate([v[1:], flip(v[:1])], axis=0)
            v = self.relax(v, up + down, f)
        return v


def ghosts(ref, rows):
    ref[0] = flip(ref[rows])
    ref[rows + 1] = flip(ref[1])


def kernel(
    nx, ny,
    forces, pressure, tables, out_p, out_r,
    fx, fy, fz, pa, g, sine, decay, rates, hartley, waves, pre, sb, rb, sb2, rb2, ex, ey,
    f0, a0, b0, f1, a1, b1, f2, a2, b2, f3, a3, b3, f4, a4,
    local_sem, plane_send, plane_recv, halo_send, halo_recv,
    go_send, go_recv, back_send, back_recv,
):
    mx, my = lax.axis_index("gx"), lax.axis_index("gy")
    n = nx * ny
    me = mx * ny + my
    bx, by, depth = pressure.shape
    tx = LANES // by
    deep = bx // (2 * tx)
    cells = bx // 2 * by

    loads = [
        pltpu.make_async_copy(forces.at[0], fx.at[pl.ds(1, bx)], local_sem.at[0]),
        pltpu.make_async_copy(forces.at[1], fy, local_sem.at[1]),
        pltpu.make_async_copy(pressure, pa.at[pl.ds(1, bx)], local_sem.at[2]),
        pltpu.make_async_copy(forces.at[2], fz, local_sem.at[3]),
    ]
    at = 0
    for ref in (sine, decay, rates, hartley, waves):
        for h in range(2):
            count, width = ref.shape[1:]
            part = tables.at[pl.ds(at, count), pl.ds(0, width)]
            loads.append(pltpu.make_async_copy(part, ref.at[h], local_sem.at[len(loads)]))
            at += count
    for load in loads:
        load.start()

    def device(d):
        return d // ny, lax.rem(d, ny)

    barrier = pltpu.get_barrier_semaphore()

    def greet(j):
        pl.semaphore_signal(
            barrier, inc=1, device_id=device(lax.rem(me + 1 + j, n)), device_id_type=MESH
        )

    loop(n - 1, greet)
    fx[0] = jnp.zeros((by, depth), jnp.float32)
    pa[0] = jnp.zeros((by, depth), jnp.float32)
    pa[bx + 1] = jnp.zeros((by, depth), jnp.float32)
    for load in loads[:3]:
        load.wait()
    pl.semaphore_wait(barrier, n - 1)

    right, left = lax.rem(mx + 1, nx), lax.rem(mx + nx - 1, nx)
    above, below = lax.rem(my + 1, ny), lax.rem(my + ny - 1, ny)

    def remote(src, dst, send, recv, to):
        copy = pltpu.make_async_remote_copy(
            src_ref=src, dst_ref=dst, send_sem=send, recv_sem=recv,
            device_id=to, device_id_type=MESH,
        )
        copy.start()
        return copy

    rows = pl.ds(1, bx)

    def strip(d, src, dst, to):
        return remote(src, dst, halo_send.at[d], halo_recv.at[d], to)

    early = [
        strip(0, pa.at[pl.ds(bx, 1)], ex.at[0, pl.ds(0, 1)], (right, my)),
        strip(1, pa.at[pl.ds(1, 1)], ex.at[0, pl.ds(1, 1)], (left, my)),
        strip(2, pa.at[rows, pl.ds(by - 1, 1)], ey.at[0, :, pl.ds(0, 1)], (mx, above)),
        strip(3, pa.at[rows, pl.ds(0, 1)], ey.at[0, :, pl.ds(SUB - 1, 1)], (mx, below)),
    ]
    early.append(
        remote(fx.at[pl.ds(bx, 1)], ex.at[1, pl.ds(0, 1)], plane_send.at[0], plane_recv.at[0], (right, my))
    )
    early.append(
        remote(
            fy.at[:, pl.ds(by - 1, 1)], ey.at[1, :, pl.ds(0, 1)],
            plane_send.at[1], plane_recv.at[1], (mx, above),
        )
    )
    for load in loads[3:]:
        load.wait()

    def make_source(i):
        r = 2 * i
        x = fx[pl.ds(r, 3)]
        y = fy[pl.ds(r, 2)]
        z = fz[pl.ds(r, 2)]
        p = pa[pl.ds(r, 4)]
        c = p[1:-1]
        lane = lax.broadcasted_iota(jnp.int32, z.shape, 2)
        column = lax.broadcasted_iota(jnp.int32, z.shape, 1)
        behind_z = jnp.where(lane == 0, 0.0, pltpu.roll(z, 1, 2))
        behind_y = jnp.where(column == 0, 0.0, pltpu.roll(y, 1, 1))
        source = (x[:-1] - x[1:]) + (behind_y - y) + (behind_z - z)
        before = jnp.where(column == 0, 0.0, pltpu.roll(c, 1, 1))
        after = jnp.where(column == by - 1, 0.0, pltpu.roll(c, by - 1, 1))
        around = (p[:-2] + p[2:]) + (before + after)
        g[pl.ds(r, 2)] = source - (4.0 * c - around)

    loop(bx // 2, make_source)

    def to_modes(matrix, rows):
        return lax.dot_general(
            matrix, rows.reshape(cells, depth), (((1,), (1,)), ((), ())),
            preferred_element_type=jnp.float32, precision=EXACT,
        )

    def prepare(q):
        h, c = q // 2, lax.rem(q, 2)
        pre[h, c] = to_modes(decay[h], pa[pl.ds(1 + c * (bx // 2), bx // 2)])

    loop(4, prepare)
    for copy in early:
        copy.wait_recv()
    g[0] += ex[0, 0] + ex[1, 0]
    g[bx - 1] += ex[0, 1]
    column = lax.broadcasted_iota(jnp.int32, (bx, SUB, depth), 1)
    g[:, 0:SUB] += jnp.where(column == 0, ey[0] + ey[1], 0.0)
    g[:, by - SUB : by] += jnp.where(column == SUB - 1, ey[0], 0.0)

    class Exchange:
        def __init__(self, h, rows, src, dst, send, recv):
            self.h, self.rows = h, pl.ds(0, rows)
            self.src, self.dst, self.send, self.recv = src, dst, send, recv

        def copy(self, src, dst, to):
            return pltpu.make_async_remote_copy(
                src_ref=src, dst_ref=dst, send_sem=self.send.at[self.h], recv_sem=self.recv.at[self.h],
                device_id=to, device_id_type=MESH,
            )

        def start(self):
            src, dst = self.src.at[self.h], self.dst.at[self.h]

            def column(i, first):
                x = mx + i
                x = jnp.where(x >= nx, x - nx, x)
                for j in range(first, ny):
                    y = my + j
                    y = jnp.where(y >= ny, y - ny, y)
                    self.copy(src.at[x * ny + y, self.rows], dst.at[me, self.rows], (x, y)).start()

            loop(nx - 1, lambda i: column(i + 1, 0))
            column(0, 1)
            self.dst[self.h, me] = self.src[self.h, me]

        def all(self):
            most = pl.ds(0, n - 1)
            return self.copy(self.src.at[self.h, most, self.rows], self.dst.at[self.h, most, self.rows], (left, my))

        def arrive(self):
            self.all().wait_recv()

        def finish(self):
            self.all().wait_send()

    def go(h):
        return Exchange(h, deep * SUB, sb, rb, go_send, go_recv)

    def back(h):
        return Exchange(h, deep * SUB + HALF, sb2, rb2, back_send, back_recv)

    def forward(h):
        modes = [to_modes(sine[h], g[pl.ds(c * (bx // 2), bx // 2)]) + pre[h, c] for c in range(2)]
        for p in range(deep):
            part = slice(p * LANES, (p + 1) * LANES)
            both = swap(*[m[:, part].reshape(n // 2, SUB, LANES) for m in modes])
            for parity in range(2):
                for e in range(n // 2):
                    sb[h, 2 * e + parity, pl.ds(p * SUB, SUB)] = both[parity][e]
        go(h).start()

    loop(2, forward)

    def solve(h):
        go(h).arrive()
        for x in range(nx // 2):
            for p in range(deep):
                pairs = [
                    swap(tile(rb, h, x * ny + y, p), tile(rb, h, (x + nx // 2) * ny + y, p)) for y in range(ny)
                ]
                for c in range(2):
                    tiles = [pair[c] for pair in pairs]
                    groups = [transposed(tiles[k : k + tx], by) for k in range(0, ny, tx)]
                    first = 1 + x * bx + c * (bx // 2) + p * tx
                    for i in range(tx):
                        f0[first + i] = jnp.concatenate([group[i] for group in groups], axis=1)
        mine = rates[h, pl.ds(pl.multiple_of(me * SUB, SUB), SUB)]
        lam = jnp.concatenate([mine] * (ny * by // LANES), axis=1)
        count = nx * bx // 2
        l0, l1, l2, l3, l4 = (Level(i, count // 2**i, lam, waves) for i in range(LEVELS))
        inner = pl.ds(1, count)

        def along_y(ref, direction):
            return lax.dot_general(
                ref[inner].reshape(count * SUB, ny * by), hartley[direction], (((1,), (0,)), ((), ())),
                preferred_element_type=jnp.float32, precision=EXACT,
            ).reshape(count, SUB, ny * by)

        f0[inner] = along_y(f0, 0)
        ghosts(f0, count)
        for cycle in range(CYCLES):
            if cycle == 0:
                l0.sweep_twice_from_zero(f0, a0)
            else:
                l0.sweep(a0, f0, b0)
                l0.sweep(b0, f0, a0)
            l0.restricted(a0, f0, f1)
            l1.sweep_twice_from_zero(f1, a1)
            l1.restricted(a1, f1, f2)
            l2.sweep_twice_from_zero(f2, a2)
            l2.restricted(a2, f2, f3)
            l3.sweep_twice_from_zero(f3, a3)
            l3.restricted(a3, f3, f4)
            a4[pl.ds(1, l4.rows)] = l4.solve(f4[pl.ds(1, l4.rows)])
            ghosts(a4, l4.rows)
            l3.corrected_sweep(a3, a4, f3, b3)
            l3.sweep(b3, f3, a3)
            l2.corrected_sweep(a2, a3, f2, b2)
            l2.sweep(b2, f2, a2)
            l1.corrected_sweep(a1, a2, f1, b1)
            l1.sweep(b1, f1, a1)
            l0.corrected_sweep(a0, a1, f0, b0)
            l0.sweep(b0, f0, a0)
        b0[inner] = along_y(a0, 1)
        for x in range(nx // 2):
            for p in range(deep):
                kept = []
                for c in range(2):
                    first = 1 + x * bx + c * (bx // 2) + p * tx
                    block = b0[pl.ds(first, tx)]
                    tiles = []
                    for k in range(ny // tx):
                        part = slice(k * LANES, (k + 1) * LANES)
                        tiles += transposed([block[i][:, part] for i in range(tx)], by)
                    kept.append(tiles)
                for y in range(ny):
                    one, other = swap(kept[0][y], kept[1][y])
                    sb2[h, x * ny + y, pl.ds(p * SUB, SUB)] = one
                    sb2[h, (x + nx // 2) * ny + y, pl.ds(p * SUB, SUB)] = other
        ghosts(b0, count)
        for x in range(nx // 2):
            lines(h, x)
        back(h).start()

    def lines(h, x):
        width = ny * by
        lane = lax.broadcasted_iota(jnp.int32, (SUB, width), 1)
        column = lax.rem(lane, by)
        first = last = jnp.zeros((SUB, width), jnp.float32)
        for i in range(bx):
            row = b0[1 + x * bx + i]
            first = jnp.where(column == i, pltpu.roll(row, i, 1), first)
            last = jnp.where(column == i, pltpu.roll(row, (i + 1 - by) % width, 1), last)
        lane = lane[:, 0:LANES]
        for y in range(ny):
            parts = [
                pltpu.roll(piece, shift % width, 1)[:, 0:LANES]
                for piece, shift in (
                    (b0[x * bx], -y * by),
                    (b0[1 + (x + 1) * bx], by - y * by),
                    (last, 2 * by - (y - 1) % ny * by),
                    (first, 2 * by + bx - (y + 1) % ny * by),
                )
            ]
            line = parts[3]
            for part, stop in zip(parts[2::-1], (2 * by + bx, 2 * by, by)):
                line = jnp.where(lane < stop, part, line)
            spot = pl.ds(deep * SUB, SUB)
            sb2[h, x * ny + y, spot] = line
            sb2[h, (x + nx // 2) * ny + y, spot] = flip(line)

    loop(2, solve)

    def to_cells(mail, h):
        parts = [[], []]
        for p in range(deep):
            tiles = [
                swap(tile(mail, h, 2 * e, p), tile(mail, h, 2 * e + 1, p)) for e in range(n // 2)
            ]
            for c in range(2):
                parts[c].append(jnp.concatenate([t[c] for t in tiles], axis=0))
        for c in range(2):
            values = lax.dot_general(
                jnp.concatenate(parts[c], axis=1), sine[h], (((0,), (0,)), ((), ())),
                preferred_element_type=jnp.float32, precision=EXACT,
            )
            yield c * (bx // 2), values.reshape(bx // 2, by, depth)

    def inner_remainder(h, d):
        c = rb2[h, d, 0 : deep * SUB].reshape(deep, SUB, LANES)
        lane = lax.broadcasted_iota(jnp.int32, c.shape, 2)
        lower = low((1, SUB, LANES))
        column = lax.rem(lane, by)
        after = pltpu.roll(c, LANES - by, 2)
        beyond = jnp.where(lower, flip(after[:1]), 0.0)
        after = jnp.where(lane < LANES - by, after, jnp.concatenate([after[1:], beyond], axis=0))
        before = pltpu.roll(c, by, 2)
        beyond = jnp.where(lower, 0.0, flip(before[-1:]))
        before = jnp.where(lane < by, jnp.concatenate([beyond, before[:-1]], axis=0), before)
        after_y = jnp.where(column == by - 1, 0.0, pltpu.roll(c, LANES - 1, 2))
        before_y = jnp.where(column == 0, 0.0, pltpu.roll(c, 1, 2))
        lam = rates[h, pl.ds(pl.multiple_of(d * SUB, SUB), SUB)][None]
        f = sb[h, d].reshape(deep, SUB, LANES)
        r = (f - lam * c) - (4.0 * c - ((after + before) + (after_y + before_y)))
        rb[h, d] = r.reshape(deep * SUB, LANES)

    def remainders(h):
        def several(i):
            for j in range(8):
                inner_remainder(h, 8 * i + j)

        loop(n // 8, several)

    def add_lines(h):
        pairs = [swap(tile(rb2, h, 2 * e, deep), tile(rb2, h, 2 * e + 1, deep)) for e in range(n // 2)]
        values = lax.dot_general(
            jnp.concatenate([pair[0] for pair in pairs], axis=0), sine[h], (((0,), (0,)), ((), ())),
            preferred_element_type=jnp.float32, precision=EXACT,
        )
        out_r[0] += values[0:by]
        out_r[bx - 1] += values[by : 2 * by]
        sub = lax.broadcasted_iota(jnp.int32, (SUB, depth), 0)
        for i in range(bx):
            at = 2 * by + i
            before = jnp.broadcast_to(values[at : at + 1], (SUB, depth))
            after = jnp.broadcast_to(values[at + bx : at + bx + 1], (SUB, depth))
            out_r[i, 0:SUB] += jnp.where(sub == 0, before, 0.0)
            out_r[i, by - SUB : by] += jnp.where(sub == SUB - 1, after, 0.0)

    half = bx // 2

    def home(h, first):
        back(h).arrive()
        for r, values in to_cells(rb2, h):
            old = pa[pl.ds(1 + r, half)] if first else out_p[pl.ds(r, half)]
            out_p[pl.ds(r, half)] = old + values
        remainders(h)
        for r, values in to_cells(rb, h):
            out_r[pl.ds(r, half)] = values if first else out_r[pl.ds(r, half)] + values
        add_lines(h)

    home(0, True)
    home(1, False)
    for copy in early:
        copy.wait_send()
    for h in range(2):
        go(h).finish()
        back(h).finish()


def transform(depth, n, width):
    per = -(-depth // n)
    each = -(-per // 2)
    index = np.arange(1, depth + 1)
    angle = np.pi / (depth + 1)
    sines = np.sqrt(2.0 / (depth + 1)) * np.sin(angle * (np.outer(index, index) % (2 * (depth + 1))))
    rates = 4.0 * np.sin(0.5 * angle * index) ** 2
    matrix = np.zeros((2, n, HALF, depth))
    column = np.ones((2, n, 2, HALF))
    decay = np.zeros((2, n, HALF, depth))
    for m in range(depth):
        d, h, j = m // per, m % per // each, m % per % each
        matrix[h, d, j] = sines[m]
        decay[h, d, j] = -rates[m] * sines[m]
        column[h, d, :, j] = rates[m]
    column = np.repeat(column.reshape(2, n * SUB, 1), LANES, axis=2)
    angle = 2 * np.pi / (2 * width) * (np.outer(np.arange(width), 2 * np.arange(width) + 1) % (2 * width))
    cas = np.cos(angle) + np.sin(angle)
    waves = np.zeros((2, LEVELS, SUB, width))
    for level in range(LEVELS):
        period = width // 2**level
        q = np.arange(width) % period
        waves[0, level] = 4.0 - 2.0 * np.cos(2 * np.pi * q / period)
        waves[1, level] = np.cos(np.pi * q / period) * np.where(2 * q < period, 1.0, -1.0)
    hartley = np.stack([cas.T / width, cas])
    return [
        matrix.reshape(2, n * HALF, depth), decay.reshape(2, n * HALF, depth), column,
        hartley, waves.reshape(2, LEVELS * SUB, width),
    ]


def stacked(arrays):
    wide = max(a.shape[2] for a in arrays)
    padded = [np.pad(a, ((0, 0), (0, 0), (0, wide - a.shape[2]))) for a in arrays]
    return np.concatenate([half for a in padded for half in a]).astype(np.float32)


def on_device(nx, ny, forces, pressure_prev):
    bx, by, depth = pressure_prev.shape
    n = nx * ny
    f32 = jnp.float32
    width = ny * by
    tx = LANES // by
    deep = bx // (2 * tx)
    constants = transform(depth, n, width)

    def vmem(*shape):
        return pltpu.VMEM(shape, f32)

    sem = pltpu.SemaphoreType.DMA
    block = (bx, by, depth)
    levels = []
    for level in range(LEVELS):
        count = 3 if level < LEVELS - 1 else 2
        levels += [vmem(nx * bx // 2 // 2**level + 2, SUB, width)] * count
    scratch = (
        [vmem(bx + 1, by, depth), vmem(*block), vmem(*block)]
        + [vmem(bx + 2, by, depth)]
        + [vmem(*block)]
        + [vmem(*c.shape) for c in constants]
        + [vmem(2, 2, n * HALF, bx // 2 * by)]
        + [vmem(2, n, deep * SUB, LANES)] * 2
        + [vmem(2, n, (deep + 1) * SUB, LANES)] * 2
        + [vmem(2, 2, by, depth), vmem(2, bx, SUB, depth)]
        + levels
        + [sem((14,)), sem((2,)), sem((2,)), sem((4,)), sem((4,))]
        + [sem((2,))] * 4
    )
    shape = jax.ShapeDtypeStruct(block, f32)
    hbmspace = pl.BlockSpec(memory_space=pltpu.HBM)
    vmemspace = pl.BlockSpec(memory_space=pltpu.VMEM)
    return pl.pallas_call(
        functools.partial(kernel, nx, ny),
        out_shape=(shape, shape),
        in_specs=[hbmspace] * 3,
        out_specs=(vmemspace, vmemspace),
        scratch_shapes=scratch,
        compiler_params=pltpu.CompilerParams(
            collective_id=0, has_side_effects=True, vmem_limit_bytes=67043328 - int(11.2 * 1024 * 1024)
        ),
    )(forces, pressure_prev, stacked(constants))


def solution(mesh):
    return jax.shard_map(
        functools.partial(on_device, mesh.shape["gx"], mesh.shape["gy"]),
        mesh=mesh,
        in_specs=(P(None, "gx", "gy", None), P("gx", "gy", None)),
        out_specs=(P("gx", "gy", None), P("gx", "gy", None)),
        check_vma=False,
    )
```

```python
import functools

import numpy as np

import jax
import jax.numpy as jnp
from jax import lax
from jax.experimental import pallas as pl
from jax.experimental.pallas import tpu as pltpu
from jax.sharding import PartitionSpec as P

OMEGA = 0.8
LEVELS = 5
CYCLES = 2
COARSE_SWEEPS = 4
SUB = 8
HALF = 4
QUARTER = 32
LANES = 128
MESH = pl.DeviceIdType.MESH
EXACT = lax.Precision.HIGHEST


def loop(count, body):
    def step(i, carry):
        body(i)
        return carry

    lax.fori_loop(0, count, step, 0)


def low(shape):
    return lax.broadcasted_iota(jnp.int32, shape, len(shape) - 2) < HALF


def flip(c):
    return pltpu.roll(c, HALF, c.ndim - 2)


def swap(a, b):
    mask = low(a.shape)
    return jnp.where(mask, a, flip(b)), jnp.where(mask, flip(a), b)


def transposed(tiles, by):
    tiles = list(tiles)
    lane = lax.broadcasted_iota(jnp.int32, tiles[0].shape, tiles[0].ndim - 1)
    axis = tiles[0].ndim - 1
    step = 1
    while step < len(tiles):
        odd = (lane & (step * by)) != 0
        for g in range(len(tiles)):
            if g & step == 0:
                a, b = tiles[g], tiles[g + step]
                tiles[g] = jnp.where(odd, pltpu.roll(b, step * by, axis), a)
                tiles[g + step] = jnp.where(odd, b, pltpu.roll(a, LANES - step * by, axis))
        step *= 2
    return tiles


def tile(mail, h, d, p):
    return mail[h, d, pl.ds(p * SUB, SUB)]


def packed(line):
    mode = lax.rem(lax.broadcasted_iota(jnp.int32, line.shape, 0), HALF)
    lane = lax.broadcasted_iota(jnp.int32, line.shape, 1)
    out = line
    for i in range(HALF - 1):
        moved = pltpu.roll(pltpu.roll(line, SUB - HALF + 1 + i, 0), (HALF - 1 - i) * QUARTER, 1)
        out = jnp.where((lane >= LANES - QUARTER) & (mode == i), moved, out)
    return out


def unpacked(line):
    mode = lax.rem(lax.broadcasted_iota(jnp.int32, line.shape, 0), HALF)
    lane = lax.broadcasted_iota(jnp.int32, line.shape, 1)
    out = line
    for i in range(HALF - 1):
        moved = pltpu.roll(pltpu.roll(line, HALF - 1 - i, 0), (i + 1) * QUARTER, 1)
        here = (lane >= i * QUARTER) & (lane < (i + 1) * QUARTER)
        out = jnp.where(here & (mode == HALF - 1), moved, out)
    return out


class Level:
    def __init__(self, index, rows, rate, waves):
        self.rows, self.rate = rows, rate
        self.width = rate.shape[1]
        self.period = self.width // 2**index
        self.weight = 0.25**index
        self.k = OMEGA / (4.0 * self.weight + 2.0)
        self.unit = min(rows, 64 * LANES // self.width)
        self.side, self.pair = (waves[i, pl.ds(index * SUB, SUB)] for i in range(2))

    def symbol(self):
        return self.k * (self.weight * self.side + self.rate)

    def relax(self, c, beside, f):
        return (1.0 - self.symbol()) * c + (self.k * self.weight) * beside + self.k * f

    def begin(self, f, beside):
        return (self.k * (2.0 - self.symbol())) * f + (self.k * self.k * self.weight) * beside

    def remainder(self, c, beside, f):
        return (f - self.rate * c) - self.weight * (self.side * c - beside)

    def restrict(self, r):
        pairs = r.reshape((r.shape[0] // 2, 2) + r.shape[1:])
        s = (0.5 * self.pair) * (pairs[:, 0] + pairs[:, 1])
        return s + pltpu.roll(s, self.period // 2, 2)

    def each(self, body):
        if self.unit == self.rows:
            body(0)
        else:
            loop(self.rows // self.unit, lambda i: body(pl.multiple_of(i * self.unit, self.unit)))

    def around(self, ref, x):
        block = ref[pl.ds(x, self.unit + 2)]
        return block[1:-1], block[:-2] + block[2:]

    def sweep(self, v, f, dst):
        def body(x):
            c, beside = self.around(v, x)
            dst[pl.ds(1 + x, self.unit)] = self.relax(c, beside, f[pl.ds(1 + x, self.unit)])

        self.each(body)
        ghosts(dst, self.rows)

    def sweep_twice_from_zero(self, f, dst):
        def body(x):
            c, beside = self.around(f, x)
            dst[pl.ds(1 + x, self.unit)] = self.begin(c, beside)

        self.each(body)
        ghosts(dst, self.rows)

    def restricted(self, v, f, dst):
        def body(x):
            c, beside = self.around(v, x)
            r = self.remainder(c, beside, f[pl.ds(1 + x, self.unit)])
            dst[pl.ds(1 + x // 2, self.unit // 2)] = self.restrict(r)

        self.each(body)
        ghosts(dst, self.rows // 2)

    def corrected_sweep(self, v, e, f, dst):
        def body(x):
            block = v[pl.ds(x, self.unit + 2)]
            half = self.pair * e[pl.ds(x // 2, self.unit // 2 + 2)]
            pieces = [half[i] for i in range(self.unit // 2 + 2)]
            twice = [pieces[0]] + [p for p in pieces[1:-1] for _ in range(2)] + [pieces[-1]]
            block = block + jnp.stack(twice)
            c, beside = block[1:-1], block[:-2] + block[2:]
            dst[pl.ds(1 + x, self.unit)] = self.relax(c, beside, f[pl.ds(1 + x, self.unit)])

        self.each(body)
        ghosts(dst, self.rows)

    def solve(self, f):
        mean = jnp.sum(f, axis=0)
        mean = (mean + flip(mean)) / (2 * self.rows)
        lane = lax.broadcasted_iota(jnp.int32, mean.shape, 1)
        mean = jnp.where(lax.rem(lane, self.period) == 0, mean / self.rate, 0.0)
        v = jnp.broadcast_to(mean[None], f.shape)
        for _ in range(COARSE_SWEEPS):
            up = jnp.concatenate([flip(v[-1:]), v[:-1]], axis=0)
            down = jnp.concatenate([v[1:], flip(v[:1])], axis=0)
            v = self.relax(v, up + down, f)
        return v


def ghosts(ref, rows):
    ref[0] = flip(ref[rows])
    ref[rows + 1] = flip(ref[1])


def kernel(
    nx, ny,
    forces, pressure, tables, out_p, out_r,
    fx, fy, fz, pa, g, sine, decay, rates, hartley, waves, pre, sb, rb, sb2, rb2, ex, ey,
    f0, a0, b0, f1, a1, b1, f2, a2, b2, f3, a3, b3, f4, a4,
    local_sem, plane_send, plane_recv, halo_send, halo_recv,
    go_send, go_recv, back_send, back_recv,
):
    mx, my = lax.axis_index("gx"), lax.axis_index("gy")
    n = nx * ny
    me = mx * ny + my
    bx, by, depth = pressure.shape
    tx = LANES // by
    deep = bx // (2 * tx)
    cells = bx // 2 * by

    loads = [
        pltpu.make_async_copy(forces.at[0], fx.at[pl.ds(1, bx)], local_sem.at[0]),
        pltpu.make_async_copy(forces.at[1], fy, local_sem.at[1]),
        pltpu.make_async_copy(pressure, pa.at[pl.ds(1, bx)], local_sem.at[2]),
        pltpu.make_async_copy(forces.at[2], fz, local_sem.at[3]),
    ]
    at = 0
    for ref in (sine, decay, rates, hartley, waves):
        for h in range(2):
            count, width = ref.shape[1:]
            part = tables.at[pl.ds(at, count), pl.ds(0, width)]
            loads.append(pltpu.make_async_copy(part, ref.at[h], local_sem.at[len(loads)]))
            at += count
    for load in loads:
        load.start()

    def device(d):
        return d // ny, lax.rem(d, ny)

    barrier = pltpu.get_barrier_semaphore()

    def greet(j):
        pl.semaphore_signal(
            barrier, inc=1, device_id=device(lax.rem(me + 1 + j, n)), device_id_type=MESH
        )

    loop(n - 1, greet)
    fx[0] = jnp.zeros((by, depth), jnp.float32)
    pa[0] = jnp.zeros((by, depth), jnp.float32)
    pa[bx + 1] = jnp.zeros((by, depth), jnp.float32)
    for load in loads[:3]:
        load.wait()
    pl.semaphore_wait(barrier, n - 1)

    right, left = lax.rem(mx + 1, nx), lax.rem(mx + nx - 1, nx)
    above, below = lax.rem(my + 1, ny), lax.rem(my + ny - 1, ny)

    def remote(src, dst, send, recv, to):
        copy = pltpu.make_async_remote_copy(
            src_ref=src, dst_ref=dst, send_sem=send, recv_sem=recv,
            device_id=to, device_id_type=MESH,
        )
        copy.start()
        return copy

    rows = pl.ds(1, bx)

    def strip(d, src, dst, to):
        return remote(src, dst, halo_send.at[d], halo_recv.at[d], to)

    early = [
        strip(0, pa.at[pl.ds(bx, 1)], ex.at[0, pl.ds(0, 1)], (right, my)),
        strip(1, pa.at[pl.ds(1, 1)], ex.at[0, pl.ds(1, 1)], (left, my)),
        strip(2, pa.at[rows, pl.ds(by - 1, 1)], ey.at[0, :, pl.ds(0, 1)], (mx, above)),
        strip(3, pa.at[rows, pl.ds(0, 1)], ey.at[0, :, pl.ds(SUB - 1, 1)], (mx, below)),
    ]
    early.append(
        remote(fx.at[pl.ds(bx, 1)], ex.at[1, pl.ds(0, 1)], plane_send.at[0], plane_recv.at[0], (right, my))
    )
    early.append(
        remote(
            fy.at[:, pl.ds(by - 1, 1)], ey.at[1, :, pl.ds(0, 1)],
            plane_send.at[1], plane_recv.at[1], (mx, above),
        )
    )
    for load in loads[3:]:
        load.wait()

    def make_source(i):
        r = 2 * i
        x = fx[pl.ds(r, 3)]
        y = fy[pl.ds(r, 2)]
        z = fz[pl.ds(r, 2)]
        p = pa[pl.ds(r, 4)]
        c = p[1:-1]
        lane = lax.broadcasted_iota(jnp.int32, z.shape, 2)
        column = lax.broadcasted_iota(jnp.int32, z.shape, 1)
        behind_z = jnp.where(lane == 0, 0.0, pltpu.roll(z, 1, 2))
        behind_y = jnp.where(column == 0, 0.0, pltpu.roll(y, 1, 1))
        source = (x[:-1] - x[1:]) + (behind_y - y) + (behind_z - z)
        before = jnp.where(column == 0, 0.0, pltpu.roll(c, 1, 1))
        after = jnp.where(column == by - 1, 0.0, pltpu.roll(c, by - 1, 1))
        around = (p[:-2] + p[2:]) + (before + after)
        g[pl.ds(r, 2)] = source - (4.0 * c - around)

    loop(bx // 2, make_source)

    def to_modes(matrix, rows):
        return lax.dot_general(
            matrix, rows.reshape(cells, depth), (((1,), (1,)), ((), ())),
            preferred_element_type=jnp.float32, precision=EXACT,
        )

    def prepare(q):
        h, c = q // 2, lax.rem(q, 2)
        pre[h, c] = to_modes(decay[h], pa[pl.ds(1 + c * (bx // 2), bx // 2)])

    loop(4, prepare)
    for copy in early:
        copy.wait_recv()
    g[0] += ex[0, 0] + ex[1, 0]
    g[bx - 1] += ex[0, 1]
    column = lax.broadcasted_iota(jnp.int32, (bx, SUB, depth), 1)
    g[:, 0:SUB] += jnp.where(column == 0, ey[0] + ey[1], 0.0)
    g[:, by - SUB : by] += jnp.where(column == SUB - 1, ey[0], 0.0)

    class Exchange:
        def __init__(self, h, rows, src, dst, send, recv):
            self.h, self.rows = h, pl.ds(0, rows)
            self.src, self.dst, self.send, self.recv = src, dst, send, recv

        def copy(self, src, dst, to):
            return pltpu.make_async_remote_copy(
                src_ref=src, dst_ref=dst, send_sem=self.send.at[self.h], recv_sem=self.recv.at[self.h],
                device_id=to, device_id_type=MESH,
            )

        def start(self):
            src, dst = self.src.at[self.h], self.dst.at[self.h]

            def column(i, first):
                x = mx + i
                x = jnp.where(x >= nx, x - nx, x)
                for j in range(first, ny):
                    y = my + j
                    y = jnp.where(y >= ny, y - ny, y)
                    self.copy(src.at[x * ny + y, self.rows], dst.at[me, self.rows], (x, y)).start()

            loop(nx - 1, lambda i: column(i + 1, 0))
            column(0, 1)
            self.dst[self.h, me] = self.src[self.h, me]

        def all(self):
            most = pl.ds(0, n - 1)
            return self.copy(self.src.at[self.h, most, self.rows], self.dst.at[self.h, most, self.rows], (left, my))

        def arrive(self):
            self.all().wait_recv()

        def finish(self):
            self.all().wait_send()

    def go(h):
        return Exchange(h, deep * SUB, sb, rb, go_send, go_recv)

    def back(h):
        return Exchange(h, deep * SUB + HALF - 1, sb2, rb2, back_send, back_recv)

    def forward(h):
        modes = [to_modes(sine[h], g[pl.ds(c * (bx // 2), bx // 2)]) + pre[h, c] for c in range(2)]
        for p in range(deep):
            part = slice(p * LANES, (p + 1) * LANES)
            both = swap(*[m[:, part].reshape(n // 2, SUB, LANES) for m in modes])
            for parity in range(2):
                for e in range(n // 2):
                    sb[h, 2 * e + parity, pl.ds(p * SUB, SUB)] = both[parity][e]
        go(h).start()

    loop(2, forward)

    def solve(h):
        go(h).arrive()
        for x in range(nx // 2):
            for p in range(deep):
                pairs = [
                    swap(tile(rb, h, x * ny + y, p), tile(rb, h, (x + nx // 2) * ny + y, p)) for y in range(ny)
                ]
                for c in range(2):
                    tiles = [pair[c] for pair in pairs]
                    groups = [transposed(tiles[k : k + tx], by) for k in range(0, ny, tx)]
                    first = 1 + x * bx + c * (bx // 2) + p * tx
                    for i in range(tx):
                        f0[first + i] = jnp.concatenate([group[i] for group in groups], axis=1)
        mine = rates[h, pl.ds(pl.multiple_of(me * SUB, SUB), SUB)]
        lam = jnp.concatenate([mine] * (ny * by // LANES), axis=1)
        count = nx * bx // 2
        l0, l1, l2, l3, l4 = (Level(i, count // 2**i, lam, waves) for i in range(LEVELS))
        inner = pl.ds(1, count)

        def along_y(ref, direction):
            return lax.dot_general(
                ref[inner].reshape(count * SUB, ny * by), hartley[direction], (((1,), (0,)), ((), ())),
                preferred_element_type=jnp.float32, precision=EXACT,
            ).reshape(count, SUB, ny * by)

        f0[inner] = along_y(f0, 0)
        ghosts(f0, count)
        for cycle in range(CYCLES):
            if cycle == 0:
                l0.sweep_twice_from_zero(f0, a0)
            else:
                l0.sweep(a0, f0, b0)
                l0.sweep(b0, f0, a0)
            l0.restricted(a0, f0, f1)
            l1.sweep_twice_from_zero(f1, a1)
            l1.restricted(a1, f1, f2)
            l2.sweep_twice_from_zero(f2, a2)
            l2.restricted(a2, f2, f3)
            l3.sweep_twice_from_zero(f3, a3)
            l3.restricted(a3, f3, f4)
            a4[pl.ds(1, l4.rows)] = l4.solve(f4[pl.ds(1, l4.rows)])
            ghosts(a4, l4.rows)
            l3.corrected_sweep(a3, a4, f3, b3)
            l3.sweep(b3, f3, a3)
            l2.corrected_sweep(a2, a3, f2, b2)
            l2.sweep(b2, f2, a2)
            l1.corrected_sweep(a1, a2, f1, b1)
            l1.sweep(b1, f1, a1)
            l0.corrected_sweep(a0, a1, f0, b0)
            l0.sweep(b0, f0, a0)
        b0[inner] = along_y(a0, 1)
        for x in range(nx // 2):
            for p in range(deep):
                kept = []
                for c in range(2):
                    first = 1 + x * bx + c * (bx // 2) + p * tx
                    block = b0[pl.ds(first, tx)]
                    tiles = []
                    for k in range(ny // tx):
                        part = slice(k * LANES, (k + 1) * LANES)
                        tiles += transposed([block[i][:, part] for i in range(tx)], by)
                    kept.append(tiles)
                for y in range(ny):
                    one, other = swap(kept[0][y], kept[1][y])
                    sb2[h, x * ny + y, pl.ds(p * SUB, SUB)] = one
                    sb2[h, (x + nx // 2) * ny + y, pl.ds(p * SUB, SUB)] = other
        ghosts(b0, count)
        for x in range(nx // 2):
            lines(h, x)
        back(h).start()

    def lines(h, x):
        width = ny * by
        lane = lax.broadcasted_iota(jnp.int32, (SUB, width), 1)
        column = lax.rem(lane, by)
        first = last = jnp.zeros((SUB, width), jnp.float32)
        for i in range(bx):
            row = b0[1 + x * bx + i]
            first = jnp.where(column == i, pltpu.roll(row, i, 1), first)
            last = jnp.where(column == i, pltpu.roll(row, (i + 1 - by) % width, 1), last)
        lane = lane[:, 0:LANES]
        for y in range(ny):
            parts = [
                pltpu.roll(piece, shift % width, 1)[:, 0:LANES]
                for piece, shift in (
                    (b0[x * bx], -y * by),
                    (b0[1 + (x + 1) * bx], by - y * by),
                    (last, 2 * by - (y - 1) % ny * by),
                    (first, 2 * by + bx - (y + 1) % ny * by),
                )
            ]
            line = parts[3]
            for part, stop in zip(parts[2::-1], (2 * by + bx, 2 * by, by)):
                line = jnp.where(lane < stop, part, line)
            line = packed(line)
            spot = pl.ds(deep * SUB, SUB)
            sb2[h, x * ny + y, spot] = line
            sb2[h, (x + nx // 2) * ny + y, spot] = flip(line)

    loop(2, solve)

    def to_cells(mail, h):
        parts = [[], []]
        for p in range(deep):
            tiles = [
                swap(tile(mail, h, 2 * e, p), tile(mail, h, 2 * e + 1, p)) for e in range(n // 2)
            ]
            for c in range(2):
                parts[c].append(jnp.concatenate([t[c] for t in tiles], axis=0))
        for c in range(2):
            values = lax.dot_general(
                jnp.concatenate(parts[c], axis=1), sine[h], (((0,), (0,)), ((), ())),
                preferred_element_type=jnp.float32, precision=EXACT,
            )
            yield c * (bx // 2), values.reshape(bx // 2, by, depth)

    def inner_remainder(h, d):
        c = rb2[h, d, 0 : deep * SUB].reshape(deep, SUB, LANES)
        lane = lax.broadcasted_iota(jnp.int32, c.shape, 2)
        lower = low((1, SUB, LANES))
        column = lax.rem(lane, by)
        after = pltpu.roll(c, LANES - by, 2)
        beyond = jnp.where(lower, flip(after[:1]), 0.0)
        after = jnp.where(lane < LANES - by, after, jnp.concatenate([after[1:], beyond], axis=0))
        before = pltpu.roll(c, by, 2)
        beyond = jnp.where(lower, 0.0, flip(before[-1:]))
        before = jnp.where(lane < by, jnp.concatenate([beyond, before[:-1]], axis=0), before)
        after_y = jnp.where(column == by - 1, 0.0, pltpu.roll(c, LANES - 1, 2))
        before_y = jnp.where(column == 0, 0.0, pltpu.roll(c, 1, 2))
        at = d * SUB if isinstance(d, int) else pl.multiple_of(d * SUB, SUB)
        lam = rates[h, pl.ds(at, SUB)][None]
        f = sb[h, d].reshape(deep, SUB, LANES)
        r = (f - lam * c) - (4.0 * c - ((after + before) + (after_y + before_y)))
        rb[h, d] = r.reshape(deep * SUB, LANES)

    def remainders(h):
        group = min(n, 32)
        if n == group:
            for d in range(n):
                inner_remainder(h, d)
            return

        def several(i):
            for j in range(group):
                inner_remainder(h, group * i + j)

        loop(n // group, several)

    def add_lines(h):
        pairs = [swap(tile(rb2, h, 2 * e, deep), tile(rb2, h, 2 * e + 1, deep)) for e in range(n // 2)]
        values = lax.dot_general(
            jnp.concatenate([unpacked(pair[0]) for pair in pairs], axis=0), sine[h], (((0,), (0,)), ((), ())),
            preferred_element_type=jnp.float32, precision=EXACT,
        )
        out_r[0] += values[0:by]
        out_r[bx - 1] += values[by : 2 * by]
        sub = lax.broadcasted_iota(jnp.int32, (SUB, depth), 0)
        for i in range(bx):
            at = 2 * by + i
            before = jnp.broadcast_to(values[at : at + 1], (SUB, depth))
            after = jnp.broadcast_to(values[at + bx : at + bx + 1], (SUB, depth))
            out_r[i, 0:SUB] += jnp.where(sub == 0, before, 0.0)
            out_r[i, by - SUB : by] += jnp.where(sub == SUB - 1, after, 0.0)

    half = bx // 2

    def home(h, first):
        back(h).arrive()
        for r, values in to_cells(rb2, h):
            old = pa[pl.ds(1 + r, half)] if first else out_p[pl.ds(r, half)]
            out_p[pl.ds(r, half)] = old + values
        remainders(h)
        for r, values in to_cells(rb, h):
            out_r[pl.ds(r, half)] = values if first else out_r[pl.ds(r, half)] + values
        add_lines(h)

    home(0, True)
    home(1, False)
    for copy in early:
        copy.wait_send()
    for h in range(2):
        go(h).finish()
        back(h).finish()


def transform(depth, n, width):
    per = -(-depth // n)
    each = -(-per // 2)
    index = np.arange(1, depth + 1)
    angle = np.pi / (depth + 1)
    sines = np.sqrt(2.0 / (depth + 1)) * np.sin(angle * (np.outer(index, index) % (2 * (depth + 1))))
    rates = 4.0 * np.sin(0.5 * angle * index) ** 2
    matrix = np.zeros((2, n, HALF, depth))
    column = np.ones((2, n, 2, HALF))
    decay = np.zeros((2, n, HALF, depth))
    for m in range(depth):
        d, h, j = m // per, m % per // each, m % per % each
        matrix[h, d, j] = sines[m]
        decay[h, d, j] = -rates[m] * sines[m]
        column[h, d, :, j] = rates[m]
    column = np.repeat(column.reshape(2, n * SUB, 1), LANES, axis=2)
    angle = 2 * np.pi / (2 * width) * (np.outer(np.arange(width), 2 * np.arange(width) + 1) % (2 * width))
    cas = np.cos(angle) + np.sin(angle)
    waves = np.zeros((2, LEVELS, SUB, width))
    for level in range(LEVELS):
        period = width // 2**level
        q = np.arange(width) % period
        waves[0, level] = 4.0 - 2.0 * np.cos(2 * np.pi * q / period)
        waves[1, level] = np.cos(np.pi * q / period) * np.where(2 * q < period, 1.0, -1.0)
    hartley = np.stack([cas.T / width, cas])
    return [
        matrix.reshape(2, n * HALF, depth), decay.reshape(2, n * HALF, depth), column,
        hartley, waves.reshape(2, LEVELS * SUB, width),
    ]


def stacked(arrays):
    wide = max(a.shape[2] for a in arrays)
    padded = [np.pad(a, ((0, 0), (0, 0), (0, wide - a.shape[2]))) for a in arrays]
    return np.concatenate([half for a in padded for half in a]).astype(np.float32)


def on_device(nx, ny, forces, pressure_prev):
    bx, by, depth = pressure_prev.shape
    n = nx * ny
    f32 = jnp.float32
    width = ny * by
    tx = LANES // by
    deep = bx // (2 * tx)
    constants = transform(depth, n, width)

    def vmem(*shape):
        return pltpu.VMEM(shape, f32)

    sem = pltpu.SemaphoreType.DMA
    block = (bx, by, depth)
    levels = []
    for level in range(LEVELS):
        count = 3 if level < LEVELS - 1 else 2
        levels += [vmem(nx * bx // 2 // 2**level + 2, SUB, width)] * count
    scratch = (
        [vmem(bx + 1, by, depth), vmem(*block), vmem(*block)]
        + [vmem(bx + 2, by, depth)]
        + [vmem(*block)]
        + [vmem(*c.shape) for c in constants]
        + [vmem(2, 2, n * HALF, bx // 2 * by)]
        + [vmem(2, n, deep * SUB, LANES)] * 2
        + [vmem(2, n, (deep + 1) * SUB, LANES)] * 2
        + [vmem(2, 2, by, depth), vmem(2, bx, SUB, depth)]
        + levels
        + [sem((14,)), sem((2,)), sem((2,)), sem((4,)), sem((4,))]
        + [sem((2,))] * 4
    )
    shape = jax.ShapeDtypeStruct(block, f32)
    hbmspace = pl.BlockSpec(memory_space=pltpu.HBM)
    vmemspace = pl.BlockSpec(memory_space=pltpu.VMEM)
    return pl.pallas_call(
        functools.partial(kernel, nx, ny),
        out_shape=(shape, shape),
        in_specs=[hbmspace] * 3,
        out_specs=(vmemspace, vmemspace),
        scratch_shapes=scratch,
        compiler_params=pltpu.CompilerParams(
            collective_id=0, has_side_effects=True, vmem_limit_bytes=67043328 - int(11.2 * 1024 * 1024)
        ),
    )(forces, pressure_prev, stacked(constants))


def solution(mesh):
    return jax.shard_map(
        functools.partial(on_device, mesh.shape["gx"], mesh.shape["gy"]),
        mesh=mesh,
        in_specs=(P(None, "gx", "gy", None), P("gx", "gy", None)),
        out_specs=(P("gx", "gy", None), P("gx", "gy", None)),
        check_vma=False,
    )
```

```python
import functools

import numpy as np

import jax
import jax.numpy as jnp
from jax import lax
from jax.experimental import pallas as pl
from jax.experimental.pallas import tpu as pltpu
from jax.sharding import PartitionSpec as P

OMEGA = 0.8
LEVELS = 5
CYCLES = 2
COARSE_SWEEPS = 4
SUB = 8
HALF = 4
QUARTER = 32
LANES = 128
MESH = pl.DeviceIdType.MESH
EXACT = lax.Precision.HIGHEST


def loop(count, body):
    def step(i, carry):
        body(i)
        return carry

    lax.fori_loop(0, count, step, 0)


def low(shape):
    return lax.broadcasted_iota(jnp.int32, shape, len(shape) - 2) < HALF


def flip(c):
    return pltpu.roll(c, HALF, c.ndim - 2)


def swap(a, b):
    mask = low(a.shape)
    return jnp.where(mask, a, flip(b)), jnp.where(mask, flip(a), b)


def transposed(tiles, by):
    tiles = list(tiles)
    lane = lax.broadcasted_iota(jnp.int32, tiles[0].shape, tiles[0].ndim - 1)
    axis = tiles[0].ndim - 1
    step = 1
    while step < len(tiles):
        odd = (lane & (step * by)) != 0
        for g in range(len(tiles)):
            if g & step == 0:
                a, b = tiles[g], tiles[g + step]
                tiles[g] = jnp.where(odd, pltpu.roll(b, step * by, axis), a)
                tiles[g + step] = jnp.where(odd, b, pltpu.roll(a, LANES - step * by, axis))
        step *= 2
    return tiles


def tile(mail, h, d, p):
    return mail[h, d, pl.ds(p * SUB, SUB)]


def packed(line):
    mode = lax.rem(lax.broadcasted_iota(jnp.int32, line.shape, 0), HALF)
    lane = lax.broadcasted_iota(jnp.int32, line.shape, 1)
    out = line
    for i in range(HALF - 1):
        moved = pltpu.roll(pltpu.roll(line, SUB - HALF + 1 + i, 0), (HALF - 1 - i) * QUARTER, 1)
        out = jnp.where((lane >= LANES - QUARTER) & (mode == i), moved, out)
    return out


def unpacked(line):
    mode = lax.rem(lax.broadcasted_iota(jnp.int32, line.shape, 0), HALF)
    lane = lax.broadcasted_iota(jnp.int32, line.shape, 1)
    out = line
    for i in range(HALF - 1):
        moved = pltpu.roll(pltpu.roll(line, HALF - 1 - i, 0), (i + 1) * QUARTER, 1)
        here = (lane >= i * QUARTER) & (lane < (i + 1) * QUARTER)
        out = jnp.where(here & (mode == HALF - 1), moved, out)
    return out


class Level:
    def __init__(self, index, rows, rate, waves):
        self.rows, self.rate = rows, rate
        self.width = rate.shape[1]
        self.period = self.width // 2**index
        self.weight = 0.25**index
        self.k = OMEGA / (4.0 * self.weight + 2.0)
        self.unit = min(rows, 64 * LANES // self.width)
        self.side, self.pair = (waves[i, pl.ds(index * SUB, SUB)] for i in range(2))

    def symbol(self):
        return self.k * (self.weight * self.side + self.rate)

    def relax(self, c, beside, f):
        return (1.0 - self.symbol()) * c + (self.k * self.weight) * beside + self.k * f

    def begin(self, f, beside):
        return (self.k * (2.0 - self.symbol())) * f + (self.k * self.k * self.weight) * beside

    def remainder(self, c, beside, f):
        return (f - self.rate * c) - self.weight * (self.side * c - beside)

    def restrict(self, r):
        pairs = r.reshape((r.shape[0] // 2, 2) + r.shape[1:])
        s = (0.5 * self.pair) * (pairs[:, 0] + pairs[:, 1])
        return s + pltpu.roll(s, self.period // 2, 2)

    def each(self, body):
        if self.unit == self.rows:
            body(0)
        else:
            loop(self.rows // self.unit, lambda i: body(pl.multiple_of(i * self.unit, self.unit)))

    def around(self, ref, x):
        block = ref[pl.ds(x, self.unit + 2)]
        return block[1:-1], block[:-2] + block[2:]

    def sweep(self, v, f, dst):
        def body(x):
            c, beside = self.around(v, x)
            dst[pl.ds(1 + x, self.unit)] = self.relax(c, beside, f[pl.ds(1 + x, self.unit)])

        self.each(body)
        ghosts(dst, self.rows)

    def sweep_twice_from_zero(self, f, dst):
        def body(x):
            c, beside = self.around(f, x)
            dst[pl.ds(1 + x, self.unit)] = self.begin(c, beside)

        self.each(body)
        ghosts(dst, self.rows)

    def restricted(self, v, f, dst):
        def body(x):
            c, beside = self.around(v, x)
            r = self.remainder(c, beside, f[pl.ds(1 + x, self.unit)])
            dst[pl.ds(1 + x // 2, self.unit // 2)] = self.restrict(r)

        self.each(body)
        ghosts(dst, self.rows // 2)

    def corrected_sweep(self, v, e, f, dst):
        def body(x):
            block = v[pl.ds(x, self.unit + 2)]
            half = self.pair * e[pl.ds(x // 2, self.unit // 2 + 2)]
            pieces = [half[i] for i in range(self.unit // 2 + 2)]
            twice = [pieces[0]] + [p for p in pieces[1:-1] for _ in range(2)] + [pieces[-1]]
            block = block + jnp.stack(twice)
            c, beside = block[1:-1], block[:-2] + block[2:]
            dst[pl.ds(1 + x, self.unit)] = self.relax(c, beside, f[pl.ds(1 + x, self.unit)])

        self.each(body)
        ghosts(dst, self.rows)

    def solve(self, f):
        mean = jnp.sum(f, axis=0)
        mean = (mean + flip(mean)) / (2 * self.rows)
        lane = lax.broadcasted_iota(jnp.int32, mean.shape, 1)
        mean = jnp.where(lax.rem(lane, self.period) == 0, mean / self.rate, 0.0)
        v = jnp.broadcast_to(mean[None], f.shape)
        for _ in range(COARSE_SWEEPS):
            up = jnp.concatenate([flip(v[-1:]), v[:-1]], axis=0)
            down = jnp.concatenate([v[1:], flip(v[:1])], axis=0)
            v = self.relax(v, up + down, f)
        return v


def ghosts(ref, rows):
    ref[0] = flip(ref[rows])
    ref[rows + 1] = flip(ref[1])


def kernel(
    nx, ny,
    forces, pressure, tables, out_p, out_r,
    fx, fy, fz, pa, g, sine, decay, rates, hartley, waves, pre, sb, rb, sb2, rb2, edge, ex, ey,
    f0, a0, b0, f1, a1, b1, f2, a2, b2, f3, a3, b3, f4, a4,
    local_sem, halo_send, halo_recv,
    go_send, go_recv, back_send, back_recv,
):
    mx, my = lax.axis_index("gx"), lax.axis_index("gy")
    n = nx * ny
    me = mx * ny + my
    bx, by, depth = pressure.shape
    tx = LANES // by
    deep = bx // (2 * tx)
    cells = bx // 2 * by

    loads = [
        pltpu.make_async_copy(forces.at[0], fx.at[pl.ds(1, bx)], local_sem.at[0]),
        pltpu.make_async_copy(forces.at[1], fy, local_sem.at[1]),
        pltpu.make_async_copy(pressure, pa.at[pl.ds(1, bx)], local_sem.at[2]),
        pltpu.make_async_copy(forces.at[2], fz, local_sem.at[3]),
    ]
    at = 0
    for ref in (sine, decay, rates, hartley, waves):
        for h in range(2):
            count, width = ref.shape[1:]
            part = tables.at[pl.ds(at, count), pl.ds(0, width)]
            loads.append(pltpu.make_async_copy(part, ref.at[h], local_sem.at[len(loads)]))
            at += count
    for load in loads:
        load.start()

    def device(d):
        return d // ny, lax.rem(d, ny)

    barrier = pltpu.get_barrier_semaphore()

    def greet(j):
        pl.semaphore_signal(
            barrier, inc=1, device_id=device(lax.rem(me + 1 + j, n)), device_id_type=MESH
        )

    loop(n - 1, greet)
    fx[0] = jnp.zeros((by, depth), jnp.float32)
    pa[0] = jnp.zeros((by, depth), jnp.float32)
    pa[bx + 1] = jnp.zeros((by, depth), jnp.float32)
    for load in loads[:3]:
        load.wait()
    edge[0] = pa[bx] + fx[bx]
    pl.semaphore_wait(barrier, n - 1)

    right, left = lax.rem(mx + 1, nx), lax.rem(mx + nx - 1, nx)
    above, below = lax.rem(my + 1, ny), lax.rem(my + ny - 1, ny)

    def remote(src, dst, send, recv, to):
        copy = pltpu.make_async_remote_copy(
            src_ref=src, dst_ref=dst, send_sem=send, recv_sem=recv,
            device_id=to, device_id_type=MESH,
        )
        copy.start()
        return copy

    rows = pl.ds(1, bx)

    def strip(d, src, dst, to):
        return remote(src, dst, halo_send.at[d], halo_recv.at[d], to)

    early = [
        strip(0, edge, ex.at[pl.ds(0, 1)], (right, my)),
        strip(1, pa.at[pl.ds(1, 1)], ex.at[pl.ds(1, 1)], (left, my)),
        strip(2, pa.at[rows, pl.ds(by - 1, 1)], ey.at[0, :, pl.ds(0, 1)], (mx, above)),
        strip(3, pa.at[rows, pl.ds(0, 1)], ey.at[0, :, pl.ds(SUB - 1, 1)], (mx, below)),
    ]
    early.append(
        remote(
            fy.at[:, pl.ds(by - 1, 1)], ey.at[1, :, pl.ds(0, 1)],
            halo_send.at[4], halo_recv.at[4], (mx, above),
        )
    )
    for load in loads[3:]:
        load.wait()

    def make_source(i):
        r = 2 * i
        x = fx[pl.ds(r, 3)]
        y = fy[pl.ds(r, 2)]
        z = fz[pl.ds(r, 2)]
        p = pa[pl.ds(r, 4)]
        c = p[1:-1]
        lane = lax.broadcasted_iota(jnp.int32, z.shape, 2)
        column = lax.broadcasted_iota(jnp.int32, z.shape, 1)
        behind_z = jnp.where(lane == 0, 0.0, pltpu.roll(z, 1, 2))
        behind_y = jnp.where(column == 0, 0.0, pltpu.roll(y, 1, 1))
        source = (x[:-1] - x[1:]) + (behind_y - y) + (behind_z - z)
        before = jnp.where(column == 0, 0.0, pltpu.roll(c, 1, 1))
        after = jnp.where(column == by - 1, 0.0, pltpu.roll(c, by - 1, 1))
        around = (p[:-2] + p[2:]) + (before + after)
        g[pl.ds(r, 2)] = source - (4.0 * c - around)

    loop(bx // 2, make_source)

    def to_modes(matrix, rows):
        return lax.dot_general(
            matrix, rows.reshape(cells, depth), (((1,), (1,)), ((), ())),
            preferred_element_type=jnp.float32, precision=EXACT,
        )

    def prepare(q):
        h, c = q // 2, lax.rem(q, 2)
        pre[h, c] = to_modes(decay[h], pa[pl.ds(1 + c * (bx // 2), bx // 2)])

    loop(4, prepare)
    for copy in early:
        copy.wait_recv()
    g[0] += ex[0]
    g[bx - 1] += ex[1]
    column = lax.broadcasted_iota(jnp.int32, (bx, SUB, depth), 1)
    g[:, 0:SUB] += jnp.where(column == 0, ey[0] + ey[1], 0.0)
    g[:, by - SUB : by] += jnp.where(column == SUB - 1, ey[0], 0.0)

    class Exchange:
        def __init__(self, h, rows, src, dst, send, recv):
            self.h, self.rows = h, pl.ds(0, rows)
            self.src, self.dst, self.send, self.recv = src, dst, send, recv

        def copy(self, src, dst, to):
            return pltpu.make_async_remote_copy(
                src_ref=src, dst_ref=dst, send_sem=self.send.at[self.h], recv_sem=self.recv.at[self.h],
                device_id=to, device_id_type=MESH,
            )

        def start(self):
            src, dst = self.src.at[self.h], self.dst.at[self.h]

            def column(i, first):
                x = mx + i
                x = jnp.where(x >= nx, x - nx, x)
                for j in range(first, ny):
                    y = my + j
                    y = jnp.where(y >= ny, y - ny, y)
                    self.copy(src.at[x * ny + y, self.rows], dst.at[me, self.rows], (x, y)).start()

            loop(nx - 1, lambda i: column(i + 1, 0))
            column(0, 1)
            self.dst[self.h, me] = self.src[self.h, me]

        def all(self):
            most = pl.ds(0, n - 1)
            return self.copy(self.src.at[self.h, most, self.rows], self.dst.at[self.h, most, self.rows], (left, my))

        def arrive(self):
            self.all().wait_recv()

        def finish(self):
            self.all().wait_send()

    def go(h):
        return Exchange(h, deep * SUB, sb, rb, go_send, go_recv)

    def back(h):
        return Exchange(h, deep * SUB + HALF - 1, sb2, rb2, back_send, back_recv)

    def forward(h):
        modes = [to_modes(sine[h], g[pl.ds(c * (bx // 2), bx // 2)]) + pre[h, c] for c in range(2)]
        for p in range(deep):
            part = slice(p * LANES, (p + 1) * LANES)
            both = swap(*[m[:, part].reshape(n // 2, SUB, LANES) for m in modes])
            for parity in range(2):
                for e in range(n // 2):
                    sb[h, 2 * e + parity, pl.ds(p * SUB, SUB)] = both[parity][e]
        go(h).start()

    loop(2, forward)

    def solve(h):
        go(h).arrive()
        for x in range(nx // 2):
            for p in range(deep):
                pairs = [
                    swap(tile(rb, h, x * ny + y, p), tile(rb, h, (x + nx // 2) * ny + y, p)) for y in range(ny)
                ]
                for c in range(2):
                    tiles = [pair[c] for pair in pairs]
                    groups = [transposed(tiles[k : k + tx], by) for k in range(0, ny, tx)]
                    first = 1 + x * bx + c * (bx // 2) + p * tx
                    for i in range(tx):
                        f0[first + i] = jnp.concatenate([group[i] for group in groups], axis=1)
        mine = rates[h, pl.ds(pl.multiple_of(me * SUB, SUB), SUB)]
        lam = jnp.concatenate([mine] * (ny * by // LANES), axis=1)
        count = nx * bx // 2
        l0, l1, l2, l3, l4 = (Level(i, count // 2**i, lam, waves) for i in range(LEVELS))
        inner = pl.ds(1, count)

        def along_y(ref, direction):
            return lax.dot_general(
                ref[inner].reshape(count * SUB, ny * by), hartley[direction], (((1,), (0,)), ((), ())),
                preferred_element_type=jnp.float32, precision=EXACT,
            ).reshape(count, SUB, ny * by)

        f0[inner] = along_y(f0, 0)
        ghosts(f0, count)
        for cycle in range(CYCLES):
            if cycle == 0:
                l0.sweep_twice_from_zero(f0, a0)
            else:
                l0.sweep(a0, f0, b0)
                l0.sweep(b0, f0, a0)
            l0.restricted(a0, f0, f1)
            l1.sweep_twice_from_zero(f1, a1)
            l1.restricted(a1, f1, f2)
            l2.sweep_twice_from_zero(f2, a2)
            l2.restricted(a2, f2, f3)
            l3.sweep_twice_from_zero(f3, a3)
            l3.restricted(a3, f3, f4)
            a4[pl.ds(1, l4.rows)] = l4.solve(f4[pl.ds(1, l4.rows)])
            ghosts(a4, l4.rows)
            l3.corrected_sweep(a3, a4, f3, b3)
            l3.sweep(b3, f3, a3)
            l2.corrected_sweep(a2, a3, f2, b2)
            l2.sweep(b2, f2, a2)
            l1.corrected_sweep(a1, a2, f1, b1)
            l1.sweep(b1, f1, a1)
            l0.corrected_sweep(a0, a1, f0, b0)
            l0.sweep(b0, f0, a0)
        b0[inner] = along_y(a0, 1)
        for x in range(nx // 2):
            for p in range(deep):
                kept = []
                for c in range(2):
                    first = 1 + x * bx + c * (bx // 2) + p * tx
                    block = b0[pl.ds(first, tx)]
                    tiles = []
                    for k in range(ny // tx):
                        part = slice(k * LANES, (k + 1) * LANES)
                        tiles += transposed([block[i][:, part] for i in range(tx)], by)
                    kept.append(tiles)
                for y in range(ny):
                    one, other = swap(kept[0][y], kept[1][y])
                    sb2[h, x * ny + y, pl.ds(p * SUB, SUB)] = one
                    sb2[h, (x + nx // 2) * ny + y, pl.ds(p * SUB, SUB)] = other
        ghosts(b0, count)
        for x in range(nx // 2):
            lines(h, x)
        back(h).start()

    def lines(h, x):
        width = ny * by
        lane = lax.broadcasted_iota(jnp.int32, (SUB, width), 1)
        column = lax.rem(lane, by)
        first = last = jnp.zeros((SUB, width), jnp.float32)
        for i in range(bx):
            row = b0[1 + x * bx + i]
            first = jnp.where(column == i, pltpu.roll(row, i, 1), first)
            last = jnp.where(column == i, pltpu.roll(row, (i + 1 - by) % width, 1), last)
        lane = lane[:, 0:LANES]
        for y in range(ny):
            parts = [
                pltpu.roll(piece, shift % width, 1)[:, 0:LANES]
                for piece, shift in (
                    (b0[x * bx], -y * by),
                    (b0[1 + (x + 1) * bx], by - y * by),
                    (last, 2 * by - (y - 1) % ny * by),
                    (first, 2 * by + bx - (y + 1) % ny * by),
                )
            ]
            line = parts[3]
            for part, stop in zip(parts[2::-1], (2 * by + bx, 2 * by, by)):
                line = jnp.where(lane < stop, part, line)
            line = packed(line)
            spot = pl.ds(deep * SUB, SUB)
            sb2[h, x * ny + y, spot] = line
            sb2[h, (x + nx // 2) * ny + y, spot] = flip(line)

    loop(2, solve)

    def to_cells(mail, h):
        parts = [[], []]
        for p in range(deep):
            tiles = [
                swap(tile(mail, h, 2 * e, p), tile(mail, h, 2 * e + 1, p)) for e in range(n // 2)
            ]
            for c in range(2):
                parts[c].append(jnp.concatenate([t[c] for t in tiles], axis=0))
        for c in range(2):
            values = lax.dot_general(
                jnp.concatenate(parts[c], axis=1), sine[h], (((0,), (0,)), ((), ())),
                preferred_element_type=jnp.float32, precision=EXACT,
            )
            yield c * (bx // 2), values.reshape(bx // 2, by, depth)

    def inner_remainder(h, d):
        c = rb2[h, d, 0 : deep * SUB].reshape(deep, SUB, LANES)
        lane = lax.broadcasted_iota(jnp.int32, c.shape, 2)
        lower = low((1, SUB, LANES))
        column = lax.rem(lane, by)
        after = pltpu.roll(c, LANES - by, 2)
        beyond = jnp.where(lower, flip(after[:1]), 0.0)
        after = jnp.where(lane < LANES - by, after, jnp.concatenate([after[1:], beyond], axis=0))
        before = pltpu.roll(c, by, 2)
        beyond = jnp.where(lower, 0.0, flip(before[-1:]))
        before = jnp.where(lane < by, jnp.concatenate([beyond, before[:-1]], axis=0), before)
        after_y = jnp.where(column == by - 1, 0.0, pltpu.roll(c, LANES - 1, 2))
        before_y = jnp.where(column == 0, 0.0, pltpu.roll(c, 1, 2))
        at = d * SUB if isinstance(d, int) else pl.multiple_of(d * SUB, SUB)
        lam = rates[h, pl.ds(at, SUB)][None]
        f = sb[h, d].reshape(deep, SUB, LANES)
        r = (f - lam * c) - (4.0 * c - ((after + before) + (after_y + before_y)))
        rb[h, d] = r.reshape(deep * SUB, LANES)

    def remainders(h):
        group = min(n, 32)
        if n == group:
            for d in range(n):
                inner_remainder(h, d)
            return

        def several(i):
            for j in range(group):
                inner_remainder(h, group * i + j)

        loop(n // group, several)

    def add_lines(h):
        pairs = [swap(tile(rb2, h, 2 * e, deep), tile(rb2, h, 2 * e + 1, deep)) for e in range(n // 2)]
        values = lax.dot_general(
            jnp.concatenate([unpacked(pair[0]) for pair in pairs], axis=0), sine[h], (((0,), (0,)), ((), ())),
            preferred_element_type=jnp.float32, precision=EXACT,
        )
        out_r[0] += values[0:by]
        out_r[bx - 1] += values[by : 2 * by]
        sub = lax.broadcasted_iota(jnp.int32, (SUB, depth), 0)
        for i in range(bx):
            at = 2 * by + i
            before = jnp.broadcast_to(values[at : at + 1], (SUB, depth))
            after = jnp.broadcast_to(values[at + bx : at + bx + 1], (SUB, depth))
            out_r[i, 0:SUB] += jnp.where(sub == 0, before, 0.0)
            out_r[i, by - SUB : by] += jnp.where(sub == SUB - 1, after, 0.0)

    half = bx // 2

    def home(h, first):
        back(h).arrive()
        for r, values in to_cells(rb2, h):
            old = pa[pl.ds(1 + r, half)] if first else out_p[pl.ds(r, half)]
            out_p[pl.ds(r, half)] = old + values
        remainders(h)
        for r, values in to_cells(rb, h):
            out_r[pl.ds(r, half)] = values if first else out_r[pl.ds(r, half)] + values
        add_lines(h)

    home(0, True)
    home(1, False)
    for copy in early:
        copy.wait_send()
    for h in range(2):
        go(h).finish()
        back(h).finish()


def transform(depth, n, width):
    per = -(-depth // n)
    each = -(-per // 2)
    index = np.arange(1, depth + 1)
    angle = np.pi / (depth + 1)
    sines = np.sqrt(2.0 / (depth + 1)) * np.sin(angle * (np.outer(index, index) % (2 * (depth + 1))))
    rates = 4.0 * np.sin(0.5 * angle * index) ** 2
    matrix = np.zeros((2, n, HALF, depth))
    column = np.ones((2, n, 2, HALF))
    decay = np.zeros((2, n, HALF, depth))
    for m in range(depth):
        d, h, j = m // per, m % per // each, m % per % each
        matrix[h, d, j] = sines[m]
        decay[h, d, j] = -rates[m] * sines[m]
        column[h, d, :, j] = rates[m]
    column = np.repeat(column.reshape(2, n * SUB, 1), LANES, axis=2)
    angle = 2 * np.pi / (2 * width) * (np.outer(np.arange(width), 2 * np.arange(width) + 1) % (2 * width))
    cas = np.cos(angle) + np.sin(angle)
    waves = np.zeros((2, LEVELS, SUB, width))
    for level in range(LEVELS):
        period = width // 2**level
        q = np.arange(width) % period
        waves[0, level] = 4.0 - 2.0 * np.cos(2 * np.pi * q / period)
        waves[1, level] = np.cos(np.pi * q / period) * np.where(2 * q < period, 1.0, -1.0)
    hartley = np.stack([cas.T / width, cas])
    return [
        matrix.reshape(2, n * HALF, depth), decay.reshape(2, n * HALF, depth), column,
        hartley, waves.reshape(2, LEVELS * SUB, width),
    ]


def stacked(arrays):
    wide = max(a.shape[2] for a in arrays)
    padded = [np.pad(a, ((0, 0), (0, 0), (0, wide - a.shape[2]))) for a in arrays]
    return np.concatenate([half for a in padded for half in a]).astype(np.float32)


def on_device(nx, ny, forces, pressure_prev):
    bx, by, depth = pressure_prev.shape
    n = nx * ny
    f32 = jnp.float32
    width = ny * by
    tx = LANES // by
    deep = bx // (2 * tx)
    constants = transform(depth, n, width)

    def vmem(*shape):
        return pltpu.VMEM(shape, f32)

    sem = pltpu.SemaphoreType.DMA
    block = (bx, by, depth)
    levels = []
    for level in range(LEVELS):
        count = 3 if level < LEVELS - 1 else 2
        levels += [vmem(nx * bx // 2 // 2**level + 2, SUB, width)] * count
    scratch = (
        [vmem(bx + 1, by, depth), vmem(*block), vmem(*block)]
        + [vmem(bx + 2, by, depth)]
        + [vmem(*block)]
        + [vmem(*c.shape) for c in constants]
        + [vmem(2, 2, n * HALF, bx // 2 * by)]
        + [vmem(2, n, deep * SUB, LANES)] * 2
        + [vmem(2, n, (deep + 1) * SUB, LANES)] * 2
        + [vmem(1, by, depth), vmem(2, by, depth), vmem(2, bx, SUB, depth)]
        + levels
        + [sem((14,)), sem((5,)), sem((5,))]
        + [sem((2,))] * 4
    )
    shape = jax.ShapeDtypeStruct(block, f32)
    hbmspace = pl.BlockSpec(memory_space=pltpu.HBM)
    vmemspace = pl.BlockSpec(memory_space=pltpu.VMEM)
    return pl.pallas_call(
        functools.partial(kernel, nx, ny),
        out_shape=(shape, shape),
        in_specs=[hbmspace] * 3,
        out_specs=(vmemspace, vmemspace),
        scratch_shapes=scratch,
        compiler_params=pltpu.CompilerParams(
            collective_id=0, has_side_effects=True, vmem_limit_bytes=67043328 - int(11.2 * 1024 * 1024)
        ),
    )(forces, pressure_prev, stacked(constants))


def solution(mesh):
    return jax.shard_map(
        functools.partial(on_device, mesh.shape["gx"], mesh.shape["gy"]),
        mesh=mesh,
        in_specs=(P(None, "gx", "gy", None), P("gx", "gy", None)),
        out_specs=(P("gx", "gy", None), P("gx", "gy", None)),
        check_vma=False,
    )
```
